16 devices in a mesh: data: 16 (over z, y, x, core).
Axes of the slice: x: 2, y: 2, z: 2, core: 2. Of those that a mesh axis runs over, the one named last changes fastest.
Arguments:
- tokens: bfloat16 [512, 1600], P('data')
- labels: int32 [8, 512], P(None, 'data')
- w_one: bfloat16 [1600, 6400], replicated
- w_two: bfloat16 [6400, 1600], replicated
- adapter_a: bfloat16 [1600, 16], replicated
- adapter_b: bfloat16 [16, 6400], replicated
- task_heads: bfloat16 [8, 1600, 2], replicated
Outputs:
- output 1: float32 [8], replicated
- output 2: float32 [1600, 16], P('data')
- output 3: float32 [16, 6400], P(None, 'data')
All inputs are finite; a program needn't handle non-finite values.
Results may differ from the reference program's by a relative error of at most 0.00184.
Values are sent between devices in bfloat16 or wider.
A program may use at most 1 GiB of HBM per device.

```python
import jax
import jax.numpy as jnp
from jax import lax

DEVICES = 16
TOK_DEV = 32
D_MODEL = 1600
D_FF = 6400
LORA_RANK = 16
NUM_TASKS = 8
NUM_CLASSES = 2
EG_STEPS = 20


def draw_labels(label_key):
    key_list = jax.random.split(label_key, 4)
    total_tok = DEVICES * TOK_DEV
    dev_shift = jax.random.randint(key_list[0], (DEVICES, 1), 0, NUM_CLASSES)
    half_width = (NUM_CLASSES + 1) // 2
    common_lab = (dev_shift + jax.random.randint(key_list[1], (DEVICES, TOK_DEV), 0, half_width)) % NUM_CLASSES
    common_lab = common_lab.reshape(total_tok)
    own_lab = jax.random.randint(key_list[2], (NUM_TASKS, total_tok), 0, NUM_CLASSES)
    pick_common = jax.random.randint(key_list[3], (NUM_TASKS, total_tok), 0, 5) < 3
    return jnp.where(pick_common, common_lab[None, :], own_lab).astype(jnp.int32)


def setup_inputs(seed: int = 0) -> dict:
    key_list = jax.random.split(jax.random.key(seed), 8)
    total_tok = DEVICES * TOK_DEV
    tokens = jax.random.normal(key_list[0], (total_tok, D_MODEL), jnp.float32)
    w_one = jax.random.normal(key_list[1], (D_MODEL, D_FF), jnp.float32) * D_MODEL ** -0.5
    w_two = jax.random.normal(key_list[2], (D_FF, D_MODEL), jnp.float32) * D_FF ** -0.5
    adapter_a = jax.random.normal(key_list[3], (D_MODEL, LORA_RANK), jnp.float32) * D_MODEL ** -0.5
    adapter_b = jax.random.normal(key_list[4], (LORA_RANK, D_FF), jnp.float32) * LORA_RANK ** -0.5
    head_common = jax.random.normal(key_list[5], (D_MODEL, NUM_CLASSES), jnp.float32)
    head_own = jax.random.normal(key_list[6], (NUM_TASKS, D_MODEL, NUM_CLASSES), jnp.float32)
    head_sign = jnp.where(jnp.arange(NUM_TASKS) % 2 == 0, 1.0, -1.0)
    task_heads = (head_sign[:, None, None] * head_common[None] + 0.8 * head_own) * (1.5 * D_MODEL ** -0.5)
    labels = draw_labels(key_list[7])
    return {
        "tokens": tokens.astype(jnp.bfloat16),
        "labels": labels,
        "w_one": w_one.astype(jnp.bfloat16),
        "w_two": w_two.astype(jnp.bfloat16),
        "adapter_a": adapter_a.astype(jnp.bfloat16),
        "adapter_b": adapter_b.astype(jnp.bfloat16),
        "task_heads": task_heads.astype(jnp.bfloat16),
    }


def block_grads(tok_blk, lab_blk, w_one, w_two, adapter_a, adapter_b, task_heads):
    low_rank = jnp.dot(tok_blk, adapter_a, preferred_element_type=jnp.float32).astype(jnp.bfloat16)
    pre_act = jnp.dot(tok_blk, w_one, preferred_element_type=jnp.float32) + jnp.dot(low_rank, adapter_b, preferred_element_type=jnp.float32)
    gelu_out, gelu_slope = jax.jvp(jax.nn.gelu, (pre_act,), (jnp.ones_like(pre_act),))
    hidden = gelu_out.astype(jnp.bfloat16)
    trunk_out = (tok_blk.astype(jnp.float32) + jnp.dot(hidden, w_two, preferred_element_type=jnp.float32)).astype(jnp.bfloat16)
    logits = jnp.einsum("bd,tdc->tbc", trunk_out.astype(jnp.float32), task_heads.astype(jnp.float32))
    task_probs = jax.nn.softmax(logits, axis=-1)
    onehot = (lab_blk[:, :, None] == jnp.arange(NUM_CLASSES)[None, None, :]).astype(jnp.float32)
    logit_err = (task_probs - onehot).astype(jnp.bfloat16)
    d_trunk = jnp.einsum("tbc,tdc->tbd", logit_err.astype(jnp.float32), task_heads.astype(jnp.float32)).astype(jnp.bfloat16)
    d_hidden = jnp.einsum("tbd,fd->tbf", d_trunk.astype(jnp.float32), w_two.astype(jnp.float32))
    d_pre = (d_hidden * gelu_slope[None]).astype(jnp.bfloat16)
    part_b = jnp.einsum("br,tbf->trf", low_rank.astype(jnp.float32), d_pre.astype(jnp.float32))
    d_low = jnp.einsum("tbf,rf->tbr", d_pre.astype(jnp.float32), adapter_b.astype(jnp.float32)).astype(jnp.bfloat16)
    part_a = jnp.einsum("bd,tbr->tdr", tok_blk.astype(jnp.float32), d_low.astype(jnp.float32))
    return part_a, part_b


def reference(tokens, labels, w_one, w_two, adapter_a, adapter_b, task_heads):
    tok_blocks = tokens.reshape(DEVICES, TOK_DEV, D_MODEL)
    lab_blocks = labels.reshape(NUM_TASKS, DEVICES, TOK_DEV).transpose(1, 0, 2)

    def add_block(run_sum, block_in):
        part_a, part_b = block_grads(block_in[0], block_in[1], w_one, w_two, adapter_a, adapter_b, task_heads)
        return (run_sum[0] + part_a, run_sum[1] + part_b), None

    zero_init = (jnp.zeros((NUM_TASKS, D_MODEL, LORA_RANK), jnp.float32), jnp.zeros((NUM_TASKS, LORA_RANK, D_FF), jnp.float32))
    sums, _ = lax.scan(add_block, zero_init, (tok_blocks, lab_blocks))
    batch_total = DEVICES * TOK_DEV
    grad_a = sums[0] / batch_total
    grad_b = sums[1] / batch_total
    gram_mat = jnp.einsum("tdr,sdr->ts", grad_a, grad_a) + jnp.einsum("trf,srf->ts", grad_b, grad_b)
    eg_scale = jnp.trace(gram_mat) / NUM_TASKS

    def eg_step(weights, _):
        weights = weights * jnp.exp(-jnp.sum(gram_mat * weights[None, :], axis=1) / eg_scale)
        return weights / jnp.sum(weights), None

    task_weights, _ = lax.scan(eg_step, jnp.full((NUM_TASKS,), 1.0 / NUM_TASKS, jnp.float32), None, length=EG_STEPS)
    comb_a = jnp.sum(task_weights[:, None, None] * grad_a, axis=0)
    comb_b = jnp.sum(task_weights[:, None, None] * grad_b, axis=0)
    return (task_weights, comb_a, comb_b)
```

```python
import jax
import jax.numpy as jnp
from jax import lax
from jax.experimental import pallas as pl
from jax.experimental.pallas import tpu as pltpu
from jax.sharding import PartitionSpec as P

EG_STEPS = 20
F32 = jnp.float32
BF16 = jnp.bfloat16
MESH = pl.DeviceIdType.MESH

N_CHIP, N_CORE = 8, 2
TOK = 32
D, FF, R, T, C = 1600, 6400, 16, 8, 2
DP = 1664
HALF = FF // N_CORE
BLK = FF // N_CHIP
OWN = BLK // N_CORE
WIN = 896
OWIN = 512
W1_CHUNKS = ((0, 768), (768, 768), (1536, 768), (2304, 896))
W2_CHUNKS = ((0, 512), (512, 512), (1024, 512), (1536, 128))
ORDER = (1, 3, 5, 7, 6, 2, 4, 0)
GELU_C = 0.7978845608028654
N_TILE = 256


def nt(a, b):
    return lax.dot_general(a, b, (((1,), (1,)), ((), ())), preferred_element_type=F32)


def tn(a, b):
    return lax.dot_general(a, b, (((0,), (0,)), ((), ())), preferred_element_type=F32)


def nn(a, b):
    return jnp.dot(a, b, preferred_element_type=F32)


def gelu(p):
    th = jnp.tanh(GELU_C * (p + 0.044715 * (p * p * p)))
    return p * (0.5 * (1.0 + th))


def gelu_slope(p):
    p2 = p * p
    th = jnp.tanh(GELU_C * (p + 0.044715 * (p2 * p)))
    return 0.5 * (1.0 + th) + (0.5 * p * (1.0 - th * th)) * (GELU_C * (1.0 + 0.134145 * p2))


def iota(shape, dim):
    return lax.broadcasted_iota(jnp.int32, shape, dim)


def gram_parts(blocks):
    acc = [None] * 5
    for v in blocks:
        for k in range(5):
            w = v * (v if k == 0 else pltpu.roll(v, k, 0))
            w = sum(w[:, i : i + 128] for i in range(0, w.shape[1], 128))
            acc[k] = w if acc[k] is None else acc[k] + w
    return acc


def kernel(
    x_hbm, lab_hbm, w1_hbm, w2_hbm, at_hbm, bm_hbm, hd_hbm,
    alpha_out, ga_out, gb_out,
    w1h, w2h, w1w, w2w, bmh, bmw, at, hd, lab, xp, xall, hbuf, hs, ha, hb, bmt, urep, g,
    zown, zsend, zrecv, eown, eall, dz, dp, dsend, drecv, duown, duall, gb, gbrecv, mown, mall, ga,
    lsem, xs, xr, ps, pr, zs, zr, es, er, ds_, dr, bs, br, ns, nr, ms, mr, gs, gr,
):
    me = lax.axis_index("data")
    chip, core = me // N_CORE, me % N_CORE
    cx, cy, cz = chip % 2, (chip // 2) % 2, chip // 4
    mate = 1 - core

    def peer(m):
        px = 1 - cx if m & 1 else cx
        py = 1 - cy if m & 2 else cy
        pz = 1 - cz if m & 4 else cz
        return 4 * pz + 2 * py + px

    def rcopy(src, dst, ssem, rsem, chip_to, core_to):
        return pltpu.make_async_remote_copy(
            src_ref=src, dst_ref=dst, send_sem=ssem, recv_sem=rsem,
            device_id=(N_CORE * chip_to + core_to,), device_id_type=MESH,
        )

    n_sem = [0]

    def load(src, dst):
        c = pltpu.make_async_copy(src, dst, lsem.at[n_sem[0]])
        n_sem[0] += 1
        c.start()
        return c

    half0 = pl.multiple_of(core * HALF, 128)
    tile0 = (BLK * chip) // 128
    win0 = pl.multiple_of(tile0 * 128, 128)
    off = BLK * chip - win0
    c_x = load(x_hbm, xp.at[pl.ds(0, TOK)])
    c_at = load(at_hbm, at)
    c_hd = load(hd_hbm, hd)
    c_lab = load(lab_hbm, lab)
    c_bmh = load(bm_hbm.at[:, pl.ds(half0, HALF)], bmh)
    c_w1 = [load(w1_hbm.at[:, pl.ds(pl.multiple_of(half0 + a, 128), n)], w1h.at[:, pl.ds(a, n)]) for a, n in W1_CHUNKS]
    c_w2 = [
        load(w2_hbm.at[pl.ds(a, min(n, D - a)), pl.ds(half0, HALF)], w2h.at[pl.ds(a, min(n, D - a))]) for a, n in W2_CHUNKS
    ]
    c_bmw = load(bm_hbm.at[:, pl.ds(win0, WIN)], bmw)
    c_w1w = load(w1_hbm.at[:, pl.ds(win0, WIN)], w1w)
    c_w2w = load(w2_hbm.at[:, pl.ds(win0, WIN)], w2w)

    barrier = pltpu.get_barrier_semaphore()
    for m in range(N_CHIP):
        for other in range(N_CORE):
            if m or other:
                pl.semaphore_signal(
                    barrier, inc=1, device_id=(N_CORE * peer(m) + (mate if other else core),), device_id_type=MESH
                )

    hbuf[...] = jnp.zeros_like(hbuf)
    w2h[pl.ds(D, DP - D), :] = jnp.zeros((DP - D, HALF), BF16)
    eown[...] = jnp.zeros_like(eown)
    row_of_r = (iota((R, R * T), 1) // T == iota((R, R * T), 0)).astype(F32).astype(BF16)
    c_hd.wait()
    for t in range(T):
        v = hd[t].astype(F32)
        for c in range(C):
            hs[pl.ds(c * T + t, 1), :] = v[c : c + 1]
    ha[...] = hs[...].astype(BF16)
    hb[...] = jnp.concatenate([hs[T:, :], hs[:T, :]], axis=0).astype(BF16)
    c_lab.wait()
    lab_f = lab[...].astype(F32)
    eye = (iota((TOK, TOK), 0) == iota((TOK, TOK), 1)).astype(F32).astype(BF16)
    lab_t = nt(eye, jnp.concatenate([lab_f, lab_f], axis=0).astype(BF16))
    onehot = (lab_t == (iota((TOK, C * T), 1) // T).astype(F32)).astype(F32)
    c_x.wait()
    my_row = pl.multiple_of(core * (N_CHIP * TOK) + chip * TOK, TOK)
    xall[pl.ds(my_row, TOK), :] = xp[pl.ds(0, TOK), :]

    pl.semaphore_wait(barrier, N_CHIP * N_CORE - 1)

    k_xp = rcopy(xp.at[pl.ds(0, TOK)], xp.at[pl.ds(TOK, TOK)], ps, pr, chip, mate)
    k_xp.start()
    k_x = {}
    for m in (1, 2, 4, 3, 5, 6, 7):
        k_x[m] = rcopy(xp.at[pl.ds(0, TOK)], xall.at[pl.ds(my_row, TOK)], xs.at[m], xr.at[m], peer(m), core)
        k_x[m].start()

    c_at.wait()
    k_xp.wait_recv()
    x2 = xp[...]
    u2 = nt(x2, at[...]).astype(BF16)
    c_bmh.wait()
    for (a, n), cp in zip(W1_CHUNKS, c_w1):
        cp.wait()
        pre = nn(x2, w1h[:, a : a + n]) + nn(u2, bmh[:, a : a + n])
        hbuf[pl.ds(0, 2 * TOK), a : a + n] = gelu(pre).astype(BF16)
    k_z = []
    for i, ((a, n), cp) in enumerate(zip(W2_CHUNKS, c_w2)):
        cp.wait()
        zt = nt(w2h[pl.ds(a, n), :], hbuf[...])
        z = jnp.transpose(zt)
        zown[:, a : a + n] = z[:TOK]
        zsend[:, a : a + n] = z[TOK : 2 * TOK]
        k_z.append(rcopy(zsend.at[:, pl.ds(a, n)], zrecv.at[:, pl.ds(a, n)], zs.at[i], zr.at[i], chip, mate))
        k_z[-1].start()
    for k in k_z:
        k.wait_recv()
    xf = xp[pl.ds(0, TOK), :].astype(F32)
    zb = (xf + (zown[:, :D] + zrecv[:, :D])).astype(BF16)
    la, lb = nt(zb, ha[...]), nt(zb, hb[...])
    top = jnp.maximum(la, lb)
    ea, eb = jnp.exp(la - top), jnp.exp(lb - top)
    err = (ea / (ea + eb) - onehot).astype(BF16)
    eown[:, : C * T] = err
    my_slot = pl.multiple_of(chip * TOK, TOK)
    eall[pl.ds(my_slot, TOK), :] = eown[...]
    k_e = {}
    for m in (1, 2, 4, 3, 5, 6, 7):
        k_e[m] = rcopy(eown, eall.at[pl.ds(my_slot, TOK)], es.at[m], er.at[m], peer(m), core)
        k_e[m].start()

    c_bmw.wait()
    colw = iota((R, WIN), 1)
    bm_f = jnp.where((colw >= off) & (colw < off + BLK), bmw[...].astype(F32), 0.0)
    bmt[...] = tn(bm_f.astype(BF16), row_of_r).astype(BF16)
    for m in range(1, N_CHIP):
        k_x[m].wait_recv()
    grp_row = pl.multiple_of(core * (N_CHIP * TOK), N_CHIP * TOK)
    xc = xall[pl.ds(grp_row, N_CHIP * TOK), :]
    uc = nt(xc, at[...]).astype(BF16)
    urep[...] = nn(uc, row_of_r).astype(BF16)
    c_w1w.wait()
    for a in range(0, WIN, N_TILE):
        n = min(N_TILE, WIN - a)
        g[:, a : a + n] = gelu_slope(nn(xc, w1w[:, a : a + n]) + nn(uc, bmw[:, a : a + n]))
    k_g = rcopy(xall.at[pl.ds(grp_row, N_CHIP * TOK)], xall.at[pl.ds(grp_row, N_CHIP * TOK)], gs, gr, chip, mate)
    k_g.start()

    c_w2w.wait()
    lane_t = iota((TOK, R * T), 1) % T
    k_d = {}
    for step, m in enumerate(ORDER):
        buf = step % 2
        if m:
            k_e[m].wait_recv()
        slot = pl.multiple_of(peer(m) * TOK, TOK)
        e = eall[pl.ds(slot, TOK), :].astype(F32)
        for t in range(T):
            dz[buf, t * TOK : (t + 1) * TOK, :] = (
                e[:, t : t + 1] * hs[pl.ds(t, 1), :] + e[:, T + t : T + t + 1] * hs[pl.ds(T + t, 1), :]
            ).astype(BF16)
        for a in range(0, WIN, N_TILE):
            n = min(N_TILE, WIN - a)
            dh = nn(dz[buf], w2w[:, a : a + n]).reshape(T, TOK, n)
            dp[buf, :, a : a + n] = (dh * g[pl.ds(slot, TOK), a : a + n][None]).astype(BF16).reshape(T * TOK, n)
        du = nn(dp[buf], bmt[...])
        du = sum(jnp.where(lane_t == t, du[t * TOK : (t + 1) * TOK], 0.0) for t in range(T))
        if m:
            dsend[m] = du
            k_d[m] = rcopy(dsend.at[m], drecv.at[m], ds_.at[m], dr.at[m], peer(m), core)
            k_d[m].start()
        ur = urep[pl.ds(slot, TOK), :].astype(F32)
        ub = jnp.concatenate([jnp.where(lane_t == t, ur, 0.0).astype(BF16) for t in range(T)], axis=0)
        part = tn(ub, dp[buf])
        gb[...] = part if step == 0 else gb[...] + part

    ow0 = pl.multiple_of(core * (OWIN - 128), 128)
    mw0 = pl.multiple_of(mate * (OWIN - 128), 128)
    k_b = rcopy(gb.at[:, pl.ds(mw0, OWIN)], gbrecv, bs, br, chip, mate)
    k_b.start()
    for m in range(1, N_CHIP):
        k_d[m].wait_recv()
        du = du + drecv[m]
    duown[...] = du.astype(BF16)
    duall[pl.ds(my_row, TOK), :] = duown[...]
    others = [(m, o) for m in range(N_CHIP) for o in range(N_CORE) if m or o]
    k_n = []
    for i, (m, o) in enumerate(others):
        k_n.append(rcopy(duown, duall.at[pl.ds(my_row, TOK)], ns.at[i], nr.at[i], peer(m), mate if o else core))
        k_n[-1].start()

    k_b.wait_recv()
    off_own = off + 16 * core
    colo = iota((R * T, OWIN), 1)
    shard = (gb[:, pl.ds(ow0, OWIN)] + gbrecv[...]) * (1.0 / (N_CHIP * N_CORE * TOK))
    shard = jnp.where((colo >= off_own) & (colo < off_own + OWN), shard, 0.0)
    gbrecv[...] = shard
    lane = iota((T, 128), 1)
    sub = iota((T, 128), 0)
    parts = gram_parts([gbrecv[r * T : (r + 1) * T, :] for r in range(R)])
    row = sum(
        jnp.where(lane == T * k + sub, jnp.sum(p, axis=1, keepdims=True), 0.0) for k, p in enumerate(parts)
    )
    mown[...] = jnp.sum(row, axis=0, keepdims=True)
    mall[me] = mown[...]
    k_m = []
    for i, (m, o) in enumerate(others):
        k_m.append(rcopy(mown, mall.at[me], ms.at[i], mr.at[i], peer(m), mate if o else core))
        k_m[-1].start()

    k_g.wait_recv()
    for k in k_n:
        k.wait_recv()
    ga[:, :D] = tn(duall[...], xall[...]) * (1.0 / (N_CHIP * N_CORE * TOK))
    ga[:, D:] = jnp.zeros((R * T, DP - D), F32)
    parts = gram_parts([ga[r * T : (r + 1) * T, :] for r in range(R)])
    for k in k_m:
        k.wait_recv()
    mb = jnp.broadcast_to(sum(mall[i] for i in range(N_CHIP * N_CORE)), (T, 128))
    col = [
        jnp.sum(p + jnp.where(lane == T * k + sub, mb, 0.0), axis=1, keepdims=True) + jnp.zeros((T, 128), F32)
        for k, p in enumerate(parts)
    ]
    col += [pltpu.roll(col[T - k], k, 0) for k in range(5, T)]
    inv_scale = jnp.sum(col[0], axis=0, keepdims=True) / T

    def eg_step(_, w):
        grad = sum(col[k] * (w if k == 0 else pltpu.roll(w, k, 0)) for k in range(T))
        w = w * jnp.exp(-grad / inv_scale)
        return w / jnp.sum(w, axis=0, keepdims=True)

    w = lax.fori_loop(0, EG_STEPS, eg_step, jnp.full((T, 128), 1.0 / T, F32))
    alpha_out[...] = jnp.sum(jnp.where(lane == sub, w, 0.0), axis=0, keepdims=True)[:, :T]

    wcol = w[:, 0:1]
    dstart = (D // (N_CHIP * N_CORE)) * me
    dtile = dstart // 128
    da0 = pl.multiple_of(dtile * 128, 128)
    comb_a = jnp.concatenate(
        [jnp.sum(ga[r * T : (r + 1) * T, pl.ds(da0, 256)] * wcol, axis=0, keepdims=True) for r in range(R)], axis=0
    )
    ga_out[...] = pltpu.roll(comb_a, 256 - (dstart - da0), 1)[:, : D // (N_CHIP * N_CORE)]
    comb_b = jnp.concatenate(
        [jnp.sum(gbrecv[r * T : (r + 1) * T, :] * wcol, axis=0, keepdims=True) for r in range(R)], axis=0
    )
    gb_out[...] = pltpu.roll(comb_b, OWIN - off_own, 1)[:, :OWN]

    for k in [k_xp, k_g, k_b] + k_z + k_n + k_m + [k_x[m] for m in k_x] + [k_e[m] for m in k_e] + [k_d[m] for m in k_d]:
        k.wait_send()


def solution(mesh):
    n_dev = mesh.shape["data"]
    assert n_dev == N_CHIP * N_CORE
    vm = pltpu.VMEM
    dma = pltpu.SemaphoreType.DMA
    scratch = [
        vm((D, HALF), BF16), vm((DP, HALF), BF16), vm((D, WIN), BF16), vm((D, WIN), BF16),
        vm((R, HALF), BF16), vm((R, WIN), BF16), vm((R, D), BF16), vm((T, C, D), BF16), vm((T, TOK), jnp.int32),
        vm((2 * TOK, D), BF16), vm((n_dev * TOK, D), BF16), vm((128, HALF), BF16),
        vm((C * T, D), F32), vm((C * T, D), BF16), vm((C * T, D), BF16),
        vm((WIN, R * T), BF16), vm((N_CHIP * TOK, R * T), BF16), vm((N_CHIP * TOK, WIN), F32),
        vm((TOK, DP), F32), vm((TOK, DP), F32), vm((TOK, DP), F32),
        vm((TOK, 128), BF16), vm((N_CHIP * TOK, 128), BF16),
        vm((2, T * TOK, D), BF16), vm((2, T * TOK, WIN), BF16),
        vm((N_CHIP, TOK, R * T), F32), vm((N_CHIP, TOK, R * T), F32),
        vm((TOK, R * T), BF16), vm((n_dev * TOK, R * T), BF16),
        vm((R * T, WIN), F32), vm((R * T, OWIN), F32),
        vm((1, 128), F32), vm((n_dev, 1, 128), F32), vm((R * T, DP), F32),
        dma((16,)), dma((N_CHIP,)), dma((N_CHIP,)), dma, dma, dma((4,)), dma((4,)),
        dma((N_CHIP,)), dma((N_CHIP,)), dma((N_CHIP,)), dma((N_CHIP,)), dma, dma,
        dma((n_dev,)), dma((n_dev,)), dma((n_dev,)), dma((n_dev,)), dma, dma,
    ]

    def device_step(tokens, labels, w_one, w_two, adapter_a, adapter_b, task_heads):
        call = pl.pallas_call(
            kernel,
            out_shape=(
                jax.ShapeDtypeStruct((1, T), F32),
                jax.ShapeDtypeStruct((R, D // n_dev), F32),
                jax.ShapeDtypeStruct((R, FF // n_dev), F32),
            ),
            in_specs=[pl.BlockSpec(memory_space=pltpu.HBM)] * 7,
            out_specs=tuple([pl.BlockSpec(memory_space=pltpu.VMEM)] * 3),
            scratch_shapes=scratch,
            compiler_params=pltpu.CompilerParams(
                collective_id=0, has_side_effects=True, vmem_limit_bytes=60 * 1024 * 1024
            ),
            name="min_norm",
        )
        alpha, ga_t, gb = call(
            tokens, labels, w_one, w_two.T, adapter_a.T, adapter_b, task_heads.transpose(0, 2, 1)
        )
        return alpha.reshape(T), ga_t.T, gb

    return jax.shard_map(
        device_step,
        mesh=mesh,
        in_specs=(P("data", None), P(None, "data"), P(), P(), P(), P(), P()),
        out_specs=(P(), P("data", None), P(None, "data")),
        check_vma=False,
    )
```

```python
import jax
import jax.numpy as jnp
from jax import lax
from jax.experimental import pallas as pl
from jax.experimental.pallas import tpu as pltpu
from jax.sharding import PartitionSpec as P

EG_STEPS = 20
F32 = jnp.float32
BF16 = jnp.bfloat16
MESH = pl.DeviceIdType.MESH

N_CHIP, N_CORE = 8, 2
TOK = 32
D, FF, R, T, C = 1600, 6400, 16, 8, 2
DP = 1664
HALF = FF // N_CORE
BLK = FF // N_CHIP
OWN = BLK // N_CORE
WIN = 896
OWIN = 512
W1_CHUNKS = ((0, 768), (768, 768), (1536, 768), (2304, 896))
W2_CHUNKS = ((0, 512), (512, 512), (1024, 256), (1280, 320))
NEAR, FAR = (0, 1, 2, 4), (3, 5, 6, 7)
BLOCKS = ((0,), (1, 2), (3, 5, 6, 7), (4,))
GELU_C = 0.7978845608028654
N_TILE = 256


def nt(a, b):
    return lax.dot_general(a, b, (((1,), (1,)), ((), ())), preferred_element_type=F32)


def tn(a, b):
    return lax.dot_general(a, b, (((0,), (0,)), ((), ())), preferred_element_type=F32)


def nn(a, b):
    return jnp.dot(a, b, preferred_element_type=F32)


def gelu(p):
    th = jnp.tanh(GELU_C * (p + 0.044715 * (p * p * p)))
    return p * (0.5 * (1.0 + th))


def gelu_slope(p):
    p2 = p * p
    th = jnp.tanh(GELU_C * (p + 0.044715 * (p2 * p)))
    return 0.5 * (1.0 + th) + (0.5 * p * (1.0 - th * th)) * (GELU_C * (1.0 + 0.134145 * p2))


def iota(shape, dim):
    return lax.broadcasted_iota(jnp.int32, shape, dim)


def gram_parts(blocks):
    acc = [None] * 5
    for v in blocks:
        for k in range(5):
            w = v * (v if k == 0 else pltpu.roll(v, k, 0))
            w = sum(w[:, i : i + 128] for i in range(0, w.shape[1], 128))
            acc[k] = w if acc[k] is None else acc[k] + w
    return acc


def kernel(
    x_hbm, lab_hbm, w1_hbm, w2_hbm, at_hbm, bm_hbm, hd_hbm,
    alpha_out, ga_out, gb_out,
    w1h, w2h, w1w, w2w, bmh, bmw, at, hd, lab, xp, xall, hbuf, hs, ha, hb, bmt, urep, g,
    zown, zsend, zrecv, eown, eall, dz, dp, ub, dsend, drecv, duown, duall, gb, gbrecv, mown, mall, ga,
    lsem, xs, xr, ps, pr, zs, zr, es, er, ds_, dr, bs, br, ns, nr, ms, mr, gs, gr,
):
    me = lax.axis_index("data")
    chip, core = me // N_CORE, me % N_CORE
    cx, cy, cz = chip % 2, (chip // 2) % 2, chip // 4
    mate = 1 - core

    def peer(m):
        px = 1 - cx if m & 1 else cx
        py = 1 - cy if m & 2 else cy
        pz = 1 - cz if m & 4 else cz
        return 4 * pz + 2 * py + px

    def rcopy(src, dst, ssem, rsem, chip_to, core_to):
        return pltpu.make_async_remote_copy(
            src_ref=src, dst_ref=dst, send_sem=ssem, recv_sem=rsem,
            device_id=(N_CORE * chip_to + core_to,), device_id_type=MESH,
        )

    n_sem = [0]

    def load(src, dst):
        c = pltpu.make_async_copy(src, dst, lsem.at[n_sem[0]])
        n_sem[0] += 1
        c.start()
        return c

    half0 = pl.multiple_of(core * HALF, 128)
    tile0 = (BLK * chip) // 128
    win0 = pl.multiple_of(tile0 * 128, 128)
    off = BLK * chip - win0
    c_x = load(x_hbm, xp.at[pl.ds(0, TOK)])
    c_at = load(at_hbm, at)
    c_hd = load(hd_hbm, hd)
    c_lab = load(lab_hbm, lab)
    c_bmh = load(bm_hbm.at[:, pl.ds(half0, HALF)], bmh)
    c_w1 = [load(w1_hbm.at[:, pl.ds(pl.multiple_of(half0 + a, 128), n)], w1h.at[:, pl.ds(a, n)]) for a, n in W1_CHUNKS]
    c_w2 = [load(w2_hbm.at[pl.ds(a, n), pl.ds(half0, HALF)], w2h.at[pl.ds(a, n)]) for a, n in W2_CHUNKS[:-1]]
    c_bmw = load(bm_hbm.at[:, pl.ds(win0, WIN)], bmw)
    c_w1w = load(w1_hbm.at[:, pl.ds(win0, WIN)], w1w)
    c_w2 += [load(w2_hbm.at[pl.ds(a, n), pl.ds(half0, HALF)], w2h.at[pl.ds(a, n)]) for a, n in W2_CHUNKS[-1:]]
    c_w2w = load(w2_hbm.at[:, pl.ds(win0, WIN)], w2w)

    barrier = pltpu.get_barrier_semaphore()
    for m in range(N_CHIP):
        for other in range(N_CORE):
            if m or other:
                pl.semaphore_signal(
                    barrier, inc=1, device_id=(N_CORE * peer(m) + (mate if other else core),), device_id_type=MESH
                )

    eown[...] = jnp.zeros_like(eown)
    row_of_r = (iota((R, R * T), 1) // T == iota((R, R * T), 0)).astype(F32).astype(BF16)
    c_hd.wait()
    for t in range(T):
        v = hd[t].astype(F32)
        for c in range(C):
            hs[pl.ds(c * T + t, 1), :] = v[c : c + 1]
    ha[...] = hs[...].astype(BF16)
    hb[...] = jnp.concatenate([hs[T:, :], hs[:T, :]], axis=0).astype(BF16)
    c_lab.wait()
    lab_f = lab[...].astype(F32)
    eye = (iota((TOK, TOK), 0) == iota((TOK, TOK), 1)).astype(F32).astype(BF16)
    lab_t = nt(eye, jnp.concatenate([lab_f, lab_f], axis=0).astype(BF16))
    onehot = (lab_t == (iota((TOK, C * T), 1) // T).astype(F32)).astype(F32)
    c_x.wait()
    my_row = pl.multiple_of(core * (N_CHIP * TOK) + chip * TOK, TOK)
    xall[pl.ds(my_row, TOK), :] = xp[pl.ds(0, TOK), :]

    pl.semaphore_wait(barrier, N_CHIP * N_CORE - 1)

    k_xp = rcopy(xp.at[pl.ds(0, TOK)], xp.at[pl.ds(TOK, TOK)], ps, pr, chip, mate)
    k_xp.start()
    k_x = {}
    for m in (1, 2, 4, 3, 5, 6, 7):
        k_x[m] = rcopy(xp.at[pl.ds(0, TOK)], xall.at[pl.ds(my_row, TOK)], xs.at[m], xr.at[m], peer(m), core)
        k_x[m].start()

    c_at.wait()
    k_xp.wait_recv()
    x2 = xp[...]
    u2 = nt(x2, at[...]).astype(BF16)
    c_bmh.wait()
    for (a, n), cp in zip(W1_CHUNKS, c_w1):
        cp.wait()
        for i in range(a, a + n, N_TILE):
            j = min(i + N_TILE, a + n)
            pre = nn(x2, w1h[:, i:j]) + nn(u2, bmh[:, i:j])
            hbuf[:, i:j] = gelu(pre).astype(BF16)
    k_z = []
    cut = HALF // 256 * 128
    for i, ((a, n), cp) in enumerate(zip(W2_CHUNKS, c_w2)):
        cp.wait()
        if n == 2 * N_TILE:
            z = nt(hbuf[...], w2h[pl.ds(a, n), :])
        else:
            z = nt(hbuf[:, :cut], w2h[pl.ds(a, n), :cut]) + nt(hbuf[:, cut:], w2h[pl.ds(a, n), cut:])
        zown[:, a : a + n] = z[:TOK]
        zsend[:, a : a + n] = z[TOK:]
        k_z.append(rcopy(zsend.at[:, pl.ds(a, n)], zrecv.at[:, pl.ds(a, n)], zs.at[i], zr.at[i], chip, mate))
        k_z[-1].start()

    c_bmw.wait()
    colw = iota((R, WIN), 1)
    bm_f = jnp.where((colw >= off) & (colw < off + BLK), bmw[...].astype(F32), 0.0)
    bmt[...] = tn(bm_f.astype(BF16), row_of_r).astype(BF16)
    grp_row = pl.multiple_of(core * (N_CHIP * TOK), N_CHIP * TOK)
    c_w1w.wait()

    def slopes(which, base):
        for m in which:
            if m:
                k_x[m].wait_recv()
        xc = jnp.concatenate(
            [xall[pl.ds(pl.multiple_of(grp_row + peer(m) * TOK, TOK), TOK), :] for m in which], axis=0
        )
        n_row = len(which) * TOK
        uc = nt(xc, at[...]).astype(BF16)
        urep[base : base + n_row, :] = nn(uc, row_of_r).astype(BF16)
        for a in range(0, WIN, N_TILE):
            n = min(N_TILE, WIN - a)
            g[base : base + n_row, a : a + n] = gelu_slope(nn(xc, w1w[:, a : a + n]) + nn(uc, bmw[:, a : a + n]))

    slopes(NEAR, 0)
    for k in k_z:
        k.wait_recv()
    xf = xp[pl.ds(0, TOK), :].astype(F32)
    zb = (xf + (zown[...] + zrecv[...])).astype(BF16)
    la, lb = nt(zb, ha[...]), nt(zb, hb[...])
    top = jnp.maximum(la, lb)
    ea, eb = jnp.exp(la - top), jnp.exp(lb - top)
    err = (ea / (ea + eb) - onehot).astype(BF16)
    eown[:, : C * T] = err
    my_slot = pl.multiple_of(chip * TOK, TOK)
    eall[pl.ds(my_slot, TOK), :] = eown[...]
    k_e = {}
    for m in (1, 2, 4, 3, 5, 6, 7):
        k_e[m] = rcopy(eown, eall.at[pl.ds(my_slot, TOK)], es.at[m], er.at[m], peer(m), core)
        k_e[m].start()

    c_w2w.wait()
    lane_t = iota((TOK, R * T), 1) % T
    rel = {m: i * TOK for i, m in enumerate(NEAR + FAR)}
    k_d = {}

    def backward(block, first):
        for i, m in enumerate(block):
            if m:
                k_e[m].wait_recv()
        dus = {}
        for i, m in enumerate(block):
            r0 = i * T * TOK
            e = eall[pl.ds(pl.multiple_of(peer(m) * TOK, TOK), TOK), :].astype(F32)
            for t in range(T):
                dz[i, t * TOK : (t + 1) * TOK, :] = (
                    e[:, t : t + 1] * hs[pl.ds(t, 1), :] + e[:, T + t : T + t + 1] * hs[pl.ds(T + t, 1), :]
                ).astype(BF16)
            for a in range(0, WIN, N_TILE):
                n = min(N_TILE, WIN - a)
                dh = nn(dz[i], w2w[:, a : a + n]).reshape(T, TOK, n)
                slope = g[rel[m] : rel[m] + TOK, a : a + n]
                dp[r0 : r0 + T * TOK, a : a + n] = (dh * slope[None]).astype(BF16).reshape(T * TOK, n)
            du = nn(dp[r0 : r0 + T * TOK, :], bmt[...])
            dus[m] = sum(jnp.where(lane_t == t, du[t * TOK : (t + 1) * TOK], 0.0) for t in range(T))
            if m:
                dsend[m] = dus[m]
            ur = urep[rel[m] : rel[m] + TOK, :].astype(F32)
            for t in range(T):
                ub[r0 + t * TOK : r0 + (t + 1) * TOK, :] = jnp.where(lane_t == t, ur, 0.0).astype(BF16)
        n_row = len(block) * T * TOK
        for a in range(0, WIN, N_TILE):
            n = min(N_TILE, WIN - a)
            part = tn(ub[:n_row, :], dp[:n_row, a : a + n])
            gb[:, a : a + n] = part if first else gb[:, a : a + n] + part
        for m in block:
            if m:
                k_d[m] = rcopy(dsend.at[m], drecv.at[m], ds_.at[m], dr.at[m], peer(m), core)
                k_d[m].start()
        return dus

    du_own = backward(BLOCKS[0], True)[0]
    slopes(FAR, len(NEAR) * TOK)
    k_g = rcopy(xall.at[pl.ds(grp_row, N_CHIP * TOK)], xall.at[pl.ds(grp_row, N_CHIP * TOK)], gs, gr, chip, mate)
    k_g.start()
    for block in BLOCKS[1:]:
        backward(block, False)

    ow0 = pl.multiple_of(core * (OWIN - 128), 128)
    mw0 = pl.multiple_of(mate * (OWIN - 128), 128)
    k_b = rcopy(gb.at[:, pl.ds(mw0, OWIN)], gbrecv, bs, br, chip, mate)
    k_b.start()
    for m in range(1, N_CHIP):
        k_d[m].wait_recv()
        du_own = du_own + drecv[m]
    duown[...] = du_own.astype(BF16)
    duall[pl.ds(my_row, TOK), :] = duown[...]
    others = [(m, o) for m in range(N_CHIP) for o in range(N_CORE) if m or o]
    k_n = []
    for i, (m, o) in enumerate(others):
        k_n.append(rcopy(duown, duall.at[pl.ds(my_row, TOK)], ns.at[i], nr.at[i], peer(m), mate if o else core))
        k_n[-1].start()

    k_b.wait_recv()
    off_own = off + 16 * core
    colo = iota((R * T, OWIN), 1)
    shard = (gb[:, pl.ds(ow0, OWIN)] + gbrecv[...]) * (1.0 / (N_CHIP * N_CORE * TOK))
    shard = jnp.where((colo >= off_own) & (colo < off_own + OWN), shard, 0.0)
    gbrecv[...] = shard
    lane = iota((T, 128), 1)
    sub = iota((T, 128), 0)
    parts = gram_parts([gbrecv[r * T : (r + 1) * T, :] for r in range(R)])
    row = sum(
        jnp.where(lane == T * k + sub, jnp.sum(p, axis=1, keepdims=True), 0.0) for k, p in enumerate(parts)
    )
    mown[...] = jnp.sum(row, axis=0, keepdims=True)
    mall[me] = mown[...]
    k_m = []
    for i, (m, o) in enumerate(others):
        k_m.append(rcopy(mown, mall.at[me], ms.at[i], mr.at[i], peer(m), mate if o else core))
        k_m[-1].start()

    k_g.wait_recv()
    for k in k_n:
        k.wait_recv()
    ga[:, :D] = tn(duall[...], xall[...]) * (1.0 / (N_CHIP * N_CORE * TOK))
    ga[:, D:] = jnp.zeros((R * T, DP - D), F32)
    parts = gram_parts([ga[r * T : (r + 1) * T, :] for r in range(R)])
    for k in k_m:
        k.wait_recv()
    mb = jnp.broadcast_to(sum(mall[i] for i in range(N_CHIP * N_CORE)), (T, 128))
    col = [
        jnp.sum(p + jnp.where(lane == T * k + sub, mb, 0.0), axis=1, keepdims=True) + jnp.zeros((T, 128), F32)
        for k, p in enumerate(parts)
    ]
    scale = jnp.sum(col[0], axis=0, keepdims=True) / T
    col = [c / scale for c in col]
    col += [pltpu.roll(col[T - k], k, 0) for k in range(5, T)]

    def eg_step(_, w):
        grad = sum(col[k] * (w if k == 0 else pltpu.roll(w, k, 0)) for k in range(T))
        w = w * jnp.exp(-grad)
        return w / jnp.sum(w, axis=0, keepdims=True)

    w = lax.fori_loop(0, EG_STEPS, eg_step, jnp.full((T, 128), 1.0 / T, F32))
    alpha_out[...] = jnp.sum(jnp.where(lane == sub, w, 0.0), axis=0, keepdims=True)[:, :T]

    wcol = w[:, 0:1]
    dstart = (D // (N_CHIP * N_CORE)) * me
    dtile = dstart // 128
    da0 = pl.multiple_of(dtile * 128, 128)
    comb_a = jnp.concatenate(
        [jnp.sum(ga[r * T : (r + 1) * T, pl.ds(da0, 256)] * wcol, axis=0, keepdims=True) for r in range(R)], axis=0
    )
    ga_out[...] = pltpu.roll(comb_a, 256 - (dstart - da0), 1)[:, : D // (N_CHIP * N_CORE)]
    comb_b = jnp.concatenate(
        [jnp.sum(gbrecv[r * T : (r + 1) * T, :] * wcol, axis=0, keepdims=True) for r in range(R)], axis=0
    )
    gb_out[...] = pltpu.roll(comb_b, OWIN - off_own, 1)[:, :OWN]

    for k in [k_xp, k_g, k_b] + k_z + k_n + k_m + [k_x[m] for m in k_x] + [k_e[m] for m in k_e] + [k_d[m] for m in k_d]:
        k.wait_send()


def put_kernel(alpha_in, ga_in, gb_in, alpha_out, ga_out, gb_out, sem):
    pairs = ((alpha_in, alpha_out), (ga_in, ga_out), (gb_in, gb_out))
    copies = [pltpu.make_async_copy(a, b, sem.at[i]) for i, (a, b) in enumerate(pairs)]
    for c in copies:
        c.start()
    for c in copies:
        c.wait()


def solution(mesh):
    n_dev = mesh.shape["data"]
    assert n_dev == N_CHIP * N_CORE
    vm = pltpu.VMEM
    dma = pltpu.SemaphoreType.DMA
    scratch = [
        vm((D, HALF), BF16), vm((D, HALF), BF16), vm((D, WIN), BF16), vm((D, WIN), BF16),
        vm((R, HALF), BF16), vm((R, WIN), BF16), vm((R, D), BF16), vm((T, C, D), BF16), vm((T, TOK), jnp.int32),
        vm((2 * TOK, D), BF16), vm((n_dev * TOK, D), BF16), vm((2 * TOK, HALF), BF16),
        vm((C * T, D), F32), vm((C * T, D), BF16), vm((C * T, D), BF16),
        vm((WIN, R * T), BF16), vm((N_CHIP * TOK, R * T), BF16), vm((N_CHIP * TOK, WIN), F32),
        vm((TOK, D), F32), vm((TOK, D), F32), vm((TOK, D), F32),
        vm((TOK, 128), BF16), vm((N_CHIP * TOK, 128), BF16),
        vm((4, T * TOK, D), BF16), vm((4 * T * TOK, WIN), BF16), vm((4 * T * TOK, R * T), BF16),
        vm((N_CHIP, TOK, R * T), F32), vm((N_CHIP, TOK, R * T), F32),
        vm((TOK, R * T), BF16), vm((n_dev * TOK, R * T), BF16),
        vm((R * T, WIN), F32), vm((R * T, OWIN), F32),
        vm((1, 128), F32), vm((n_dev, 1, 128), F32), vm((R * T, DP), F32),
        dma((16,)), dma((N_CHIP,)), dma((N_CHIP,)), dma, dma, dma((4,)), dma((4,)),
        dma((N_CHIP,)), dma((N_CHIP,)), dma((N_CHIP,)), dma((N_CHIP,)), dma, dma,
        dma((n_dev,)), dma((n_dev,)), dma((n_dev,)), dma((n_dev,)), dma, dma,
    ]

    def device_step(tokens, labels, w_one, w_two, adapter_a, adapter_b, task_heads):
        out_shapes = ((1, T), (R, D // n_dev), (R, FF // n_dev))
        call = pl.pallas_call(
            kernel,
            out_shape=tuple(pltpu.VMEM(s, F32) for s in out_shapes),
            in_specs=[pl.BlockSpec(memory_space=pltpu.HBM)] * 7,
            out_specs=tuple([pl.BlockSpec(memory_space=pltpu.VMEM)] * 3),
            scratch_shapes=scratch,
            compiler_params=pltpu.CompilerParams(
                collective_id=0, has_side_effects=True, vmem_limit_bytes=60 * 1024 * 1024
            ),
            name="min_norm",
        )
        put = pl.pallas_call(
            put_kernel,
            out_shape=tuple(jax.ShapeDtypeStruct(s, F32) for s in out_shapes),
            in_specs=[pl.BlockSpec(memory_space=pltpu.VMEM)] * 3,
            out_specs=tuple([pl.BlockSpec(memory_space=pltpu.HBM)] * 3),
            scratch_shapes=[dma((3,))],
            compiler_params=pltpu.CompilerParams(vmem_limit_bytes=1024 * 1024),
            name="put",
        )
        results = call(
            tokens, labels, w_one, w_two.T, adapter_a.T, adapter_b, task_heads.transpose(0, 2, 1)
        )
        alpha, ga_t, gb = put(*results)
        return alpha.reshape(T), ga_t.T, gb

    return jax.shard_map(
        device_step,
        mesh=mesh,
        in_specs=(P("data", None), P(None, "data"), P(), P(), P(), P(), P()),
        out_specs=(P(), P("data", None), P(None, "data")),
        check_vma=False,
    )
```

```python
import jax
import jax.numpy as jnp
from jax import lax
from jax.experimental import pallas as pl
from jax.experimental.pallas import tpu as pltpu
from jax.sharding import PartitionSpec as P

EG_STEPS = 20
F32 = jnp.float32
BF16 = jnp.bfloat16
MESH = pl.DeviceIdType.MESH

N_CHIP, N_CORE = 8, 2
TOK = 32
D, FF, R, T, C = 1600, 6400, 16, 8, 2
DP = 1664
HALF = FF // N_CORE
BLK = FF // N_CHIP
OWN = BLK // N_CORE
WIN = 896
OWIN = 512
W1_CHUNKS = ((0, 1536), (1536, 1664))
W2_CHUNKS = ((0, 1024), (1024, 576))
NEAR, FAR = (0, 1, 2, 4), (3, 5, 6, 7)
BLOCKS = ((0,), (1, 2), (3, 5, 6, 7), (4,))
GELU_C = 0.7978845608028654
N_TILE = 256


def nt(a, b):
    return lax.dot_general(a, b, (((1,), (1,)), ((), ())), preferred_element_type=F32)


def tn(a, b):
    return lax.dot_general(a, b, (((0,), (0,)), ((), ())), preferred_element_type=F32)


def nn(a, b):
    return jnp.dot(a, b, preferred_element_type=F32)


def gelu(p):
    th = jnp.tanh(GELU_C * (p + 0.044715 * (p * p * p)))
    return p * (0.5 * (1.0 + th))


def gelu_slope(p):
    p2 = p * p
    th = jnp.tanh(GELU_C * (p + 0.044715 * (p2 * p)))
    return 0.5 * (1.0 + th) + (0.5 * p * (1.0 - th * th)) * (GELU_C * (1.0 + 0.134145 * p2))


def iota(shape, dim):
    return lax.broadcasted_iota(jnp.int32, shape, dim)


def gram_parts(blocks):
    acc = [None] * 5
    for v in blocks:
        for k in range(5):
            w = v * (v if k == 0 else pltpu.roll(v, k, 0))
            w = sum(w[:, i : i + 128] for i in range(0, w.shape[1], 128))
            acc[k] = w if acc[k] is None else acc[k] + w
    return acc


def kernel(
    x_hbm, lab_hbm, w1_hbm, w2_hbm, at_hbm, bm_hbm, hd_hbm,
    alpha_out, ga_out, gb_out,
    w1h, w2h, w1w, w2w, bmh, bmw, at, hd, lab, xp, xall, hbuf, hs, ha, hb, bmt, bms, urep, g,
    zown, zsend, zrecv, eown, eall, dz, dp, ub, dsend, drecv, duown, duall, gb, gbrecv, mown, mall, ga,
    lsem, xs, xr, ps, pr, zs, zr, es, er, ds_, dr, bs, br, ns, nr, ms, mr, gs, gr,
):
    me = lax.axis_index("data")
    chip, core = me // N_CORE, me % N_CORE
    cx, cy, cz = chip % 2, (chip // 2) % 2, chip // 4
    mate = 1 - core

    def peer(m):
        px = 1 - cx if m & 1 else cx
        py = 1 - cy if m & 2 else cy
        pz = 1 - cz if m & 4 else cz
        return 4 * pz + 2 * py + px

    def rcopy(src, dst, ssem, rsem, chip_to, core_to):
        return pltpu.make_async_remote_copy(
            src_ref=src, dst_ref=dst, send_sem=ssem, recv_sem=rsem,
            device_id=(N_CORE * chip_to + core_to,), device_id_type=MESH,
        )

    n_sem = [0]

    def load(src, dst):
        c = pltpu.make_async_copy(src, dst, lsem.at[n_sem[0]])
        n_sem[0] += 1
        c.start()
        return c

    half0 = pl.multiple_of(core * HALF, 128)
    tile0 = (BLK * chip) // 128
    win0 = pl.multiple_of(tile0 * 128, 128)
    off = BLK * chip - win0
    c_x = load(x_hbm, xp.at[pl.ds(0, TOK)])
    c_at = load(at_hbm, at)
    c_hd = load(hd_hbm, hd)
    c_lab = load(lab_hbm, lab)
    c_bmh = load(bm_hbm.at[:, pl.ds(half0, HALF)], bmh)
    c_bmw = load(bm_hbm.at[:, pl.ds(win0, WIN)], bmw)
    c_w1 = [load(w1_hbm.at[:, pl.ds(pl.multiple_of(half0 + a, 128), n)], w1h.at[:, pl.ds(a, n)]) for a, n in W1_CHUNKS]
    c_w2 = [load(w2_hbm.at[pl.ds(a, n), pl.ds(half0, HALF)], w2h.at[pl.ds(a, n)]) for a, n in W2_CHUNKS]
    c_w1w = load(w1_hbm.at[:, pl.ds(win0, WIN)], w1w.at[:, pl.ds(0, WIN)])
    c_w2w = load(w2_hbm.at[:, pl.ds(win0, WIN)], w2w)

    barrier = pltpu.get_barrier_semaphore()
    for m in range(N_CHIP):
        for other in range(N_CORE):
            if m or other:
                pl.semaphore_signal(
                    barrier, inc=1, device_id=(N_CORE * peer(m) + (mate if other else core),), device_id_type=MESH
                )

    eown[...] = jnp.zeros_like(eown)
    row_of_r = (iota((R, R * T), 1) // T == iota((R, R * T), 0)).astype(F32).astype(BF16)
    c_hd.wait()
    for t in range(T):
        v = hd[t].astype(F32)
        for c in range(C):
            hs[pl.ds(c * T + t, 1), :] = v[c : c + 1]
    ha[...] = hs[...].astype(BF16)
    hb[...] = jnp.concatenate([hs[T:, :], hs[:T, :]], axis=0).astype(BF16)
    c_lab.wait()
    lab_f = lab[...].astype(F32)
    eye = (iota((TOK, TOK), 0) == iota((TOK, TOK), 1)).astype(F32).astype(BF16)
    lab_t = nt(eye, jnp.concatenate([lab_f, lab_f], axis=0).astype(BF16))
    onehot = (lab_t == (iota((TOK, C * T), 1) // T).astype(F32)).astype(F32)
    c_x.wait()
    my_row = pl.multiple_of(core * (N_CHIP * TOK) + chip * TOK, TOK)
    xall[pl.ds(my_row, TOK), :] = xp[pl.ds(0, TOK), :]

    pl.semaphore_wait(barrier, N_CHIP * N_CORE - 1)

    k_xp = rcopy(xp.at[pl.ds(0, TOK)], xp.at[pl.ds(TOK, TOK)], ps, pr, chip, mate)
    k_xp.start()
    k_x = {}
    for m in (1, 2, 4, 3, 5, 6, 7):
        k_x[m] = rcopy(xp.at[pl.ds(0, TOK)], xall.at[pl.ds(my_row, TOK)], xs.at[m], xr.at[m], peer(m), core)
        k_x[m].start()

    c_at.wait()
    w1w[:, WIN:] = tn(at[...], row_of_r).astype(BF16)
    c_bmw.wait()
    colw = iota((R, WIN), 1)
    bm_f = jnp.where((colw >= off) & (colw < off + BLK), bmw[...].astype(F32), 0.0)
    bmt[...] = tn(bm_f.astype(BF16), row_of_r).astype(BF16)
    first_of_r = (T * iota((R, R * T), 0) == iota((R, R * T), 1)).astype(F32).astype(BF16)
    bms[...] = tn(first_of_r, bmw[...]).astype(BF16)

    k_xp.wait_recv()
    x2 = xp[...]
    u2 = nt(x2, at[...]).astype(BF16)
    c_bmh.wait()
    for (a, n), cp in zip(W1_CHUNKS, c_w1):
        cp.wait()
        for i in range(a, a + n, N_TILE):
            j = min(i + N_TILE, a + n)
            pre = nn(x2, w1h[:, i:j]) + nn(u2, bmh[:, i:j])
            hbuf[:, i:j] = gelu(pre).astype(BF16)
    k_z = []
    for i, ((a, n), cp) in enumerate(zip(W2_CHUNKS, c_w2)):
        cp.wait()
        for j in range(a, a + n, N_TILE):
            z = nt(hbuf[...], w2h[j : min(j + N_TILE, a + n), :])
            zown[:, j : min(j + N_TILE, a + n)] = z[:TOK]
            zsend[:, j : min(j + N_TILE, a + n)] = z[TOK:]
        k_z.append(rcopy(zsend.at[:, pl.ds(a, n)], zrecv.at[:, pl.ds(a, n)], zs.at[i], zr.at[i], chip, mate))
        k_z[-1].start()

    grp_row = pl.multiple_of(core * (N_CHIP * TOK), N_CHIP * TOK)
    c_w1w.wait()

    def slopes(which, base):
        for m in which:
            if m:
                k_x[m].wait_recv()
        xc = jnp.concatenate(
            [xall[pl.ds(pl.multiple_of(grp_row + peer(m) * TOK, TOK), TOK), :] for m in which], axis=0
        )
        n_row = len(which) * TOK
        last = WIN - WIN % N_TILE
        pre = nn(xc, w1w[:, last:])
        ur = pre[:, WIN - last :].astype(BF16)
        urep[base : base + n_row, :] = ur
        pre = pre[:, : WIN - last] + nn(ur, bms[:, last:])
        g[base : base + n_row, last:] = gelu_slope(pre)
        for a in range(0, last, N_TILE):
            pre = nn(xc, w1w[:, a : a + N_TILE]) + nn(ur, bms[:, a : a + N_TILE])
            g[base : base + n_row, a : a + N_TILE] = gelu_slope(pre)

    slopes(NEAR, 0)
    for k in k_z:
        k.wait_recv()
    xf = xp[pl.ds(0, TOK), :].astype(F32)
    zb = (xf + (zown[...] + zrecv[...])).astype(BF16)
    la, lb = nt(zb, ha[...]), nt(zb, hb[...])
    top = jnp.maximum(la, lb)
    ea, eb = jnp.exp(la - top), jnp.exp(lb - top)
    err = (ea / (ea + eb) - onehot).astype(BF16)
    eown[:, : C * T] = err
    my_slot = pl.multiple_of(chip * TOK, TOK)
    eall[pl.ds(my_slot, TOK), :] = eown[...]
    k_e = {}
    for m in (1, 2, 4, 3, 5, 6, 7):
        k_e[m] = rcopy(eown, eall.at[pl.ds(my_slot, TOK)], es.at[m], er.at[m], peer(m), core)
        k_e[m].start()

    c_w2w.wait()
    lane_t = iota((TOK, R * T), 1) % T
    rel = {m: i * TOK for i, m in enumerate(NEAR + FAR)}
    k_d = {}

    def backward(block):
        for m in block:
            if m:
                k_e[m].wait_recv()
        dus = {}
        for m in block:
            r0 = rel[m] * T
            e = eall[pl.ds(pl.multiple_of(peer(m) * TOK, TOK), TOK), :].astype(F32)
            for t in range(T):
                dz[rel[m] // TOK % 4, t * TOK : (t + 1) * TOK, :] = (
                    e[:, t : t + 1] * hs[pl.ds(t, 1), :] + e[:, T + t : T + t + 1] * hs[pl.ds(T + t, 1), :]
                ).astype(BF16)
            for a in range(0, WIN, N_TILE):
                n = min(N_TILE, WIN - a)
                dh = nn(dz[rel[m] // TOK % 4], w2w[:, a : a + n]).reshape(T, TOK, n)
                slope = g[rel[m] : rel[m] + TOK, a : a + n]
                dp[r0 : r0 + T * TOK, a : a + n] = (dh * slope[None]).astype(BF16).reshape(T * TOK, n)
            du = nn(dp[r0 : r0 + T * TOK, :], bmt[...])
            dus[m] = sum(jnp.where(lane_t == t, du[t * TOK : (t + 1) * TOK], 0.0) for t in range(T))
            if m:
                dsend[m] = dus[m]
            ur = urep[rel[m] : rel[m] + TOK, :].astype(F32)
            for t in range(T):
                ub[r0 + t * TOK : r0 + (t + 1) * TOK, :] = jnp.where(lane_t == t, ur, 0.0).astype(BF16)
        for m in block:
            if m:
                k_d[m] = rcopy(dsend.at[m], drecv.at[m], ds_.at[m], dr.at[m], peer(m), core)
                k_d[m].start()
        return dus

    du_own = backward(BLOCKS[0])[0]
    for block in BLOCKS[1:]:
        if block == FAR:
            slopes(FAR, len(NEAR) * TOK)
            k_g = rcopy(xall.at[pl.ds(grp_row, N_CHIP * TOK)], xall.at[pl.ds(grp_row, N_CHIP * TOK)], gs, gr, chip, mate)
            k_g.start()
        backward(block)
    for a in range(0, WIN, N_TILE):
        gb[:, a : min(a + N_TILE, WIN)] = tn(ub[...], dp[:, a : min(a + N_TILE, WIN)])

    ow0 = pl.multiple_of(core * (OWIN - 128), 128)
    mw0 = pl.multiple_of(mate * (OWIN - 128), 128)
    k_b = rcopy(gb.at[:, pl.ds(mw0, OWIN)], gbrecv, bs, br, chip, mate)
    k_b.start()
    for m in range(1, N_CHIP):
        k_d[m].wait_recv()
        du_own = du_own + drecv[m]
    duown[...] = du_own.astype(BF16)
    duall[pl.ds(my_row, TOK), :] = duown[...]
    others = [(m, o) for m in (7, 6, 5, 3, 4, 2, 1, 0) for o in range(N_CORE) if m or o]
    k_n = []
    for i, (m, o) in enumerate(others):
        k_n.append(rcopy(duown, duall.at[pl.ds(my_row, TOK)], ns.at[i], nr.at[i], peer(m), mate if o else core))
        k_n[-1].start()

    k_b.wait_recv()
    off_own = off + 16 * core
    colo = iota((R * T, OWIN), 1)
    shard = (gb[:, pl.ds(ow0, OWIN)] + gbrecv[...]) * (1.0 / (N_CHIP * N_CORE * TOK))
    shard = jnp.where((colo >= off_own) & (colo < off_own + OWN), shard, 0.0)
    gbrecv[...] = shard
    lane = iota((T, 128), 1)
    sub = iota((T, 128), 0)
    parts = gram_parts([gbrecv[r * T : (r + 1) * T, :] for r in range(R)])
    row = sum(
        jnp.where(lane == T * k + sub, jnp.sum(p, axis=1, keepdims=True), 0.0) for k, p in enumerate(parts)
    )
    mown[...] = jnp.sum(row, axis=0, keepdims=True)
    mall[me] = mown[...]
    k_m = []
    for i, (m, o) in enumerate(others):
        k_m.append(rcopy(mown, mall.at[me], ms.at[i], mr.at[i], peer(m), mate if o else core))
        k_m[-1].start()

    k_g.wait_recv()
    for k in k_n:
        k.wait_recv()
    ga[:, :D] = tn(duall[...], xall[...]) * (1.0 / (N_CHIP * N_CORE * TOK))
    ga[:, D:] = jnp.zeros((R * T, DP - D), F32)
    parts = gram_parts([ga[r * T : (r + 1) * T, :] for r in range(R)])
    for k in k_m:
        k.wait_recv()
    mb = jnp.broadcast_to(sum(mall[i] for i in range(N_CHIP * N_CORE)), (T, 128))
    col = [
        jnp.sum(p + jnp.where(lane == T * k + sub, mb, 0.0), axis=1, keepdims=True) + jnp.zeros((T, 128), F32)
        for k, p in enumerate(parts)
    ]
    scale = jnp.sum(col[0], axis=0, keepdims=True) / T
    col = [c / scale for c in col]
    col += [pltpu.roll(col[T - k], k, 0) for k in range(5, T)]

    def eg_step(_, w):
        grad = sum(col[k] * (w if k == 0 else pltpu.roll(w, k, 0)) for k in range(T))
        w = w * jnp.exp(-grad)
        return w / jnp.sum(w, axis=0, keepdims=True)

    w = lax.fori_loop(0, EG_STEPS, eg_step, jnp.full((T, 128), 1.0 / T, F32))
    alpha_out[...] = jnp.sum(jnp.where(lane == sub, w, 0.0), axis=0, keepdims=True)[:, :T]

    wcol = w[:, 0:1]
    dstart = (D // (N_CHIP * N_CORE)) * me
    dtile = dstart // 128
    da0 = pl.multiple_of(dtile * 128, 128)
    comb_a = jnp.concatenate(
        [jnp.sum(ga[r * T : (r + 1) * T, pl.ds(da0, 256)] * wcol, axis=0, keepdims=True) for r in range(R)], axis=0
    )
    ga_out[...] = pltpu.roll(comb_a, 256 - (dstart - da0), 1)[:, : D // (N_CHIP * N_CORE)]
    comb_b = jnp.concatenate(
        [jnp.sum(gbrecv[r * T : (r + 1) * T, :] * wcol, axis=0, keepdims=True) for r in range(R)], axis=0
    )
    gb_out[...] = pltpu.roll(comb_b, OWIN - off_own, 1)[:, :OWN]

    for k in [k_xp, k_g, k_b] + k_z + k_n + k_m + [k_x[m] for m in k_x] + [k_e[m] for m in k_e] + [k_d[m] for m in k_d]:
        k.wait_send()


def put_kernel(alpha_in, ga_in, gb_in, alpha_out, ga_out, gb_out, sem):
    pairs = ((alpha_in, alpha_out), (ga_in, ga_out), (gb_in, gb_out))
    copies = [pltpu.make_async_copy(a, b, sem.at[i]) for i, (a, b) in enumerate(pairs)]
    for c in copies:
        c.start()
    for c in copies:
        c.wait()


def solution(mesh):
    n_dev = mesh.shape["data"]
    assert n_dev == N_CHIP * N_CORE
    vm = pltpu.VMEM
    dma = pltpu.SemaphoreType.DMA
    scratch = [
        vm((D, HALF), BF16), vm((D, HALF), BF16), vm((D, WIN + R * T), BF16), vm((D, WIN), BF16),
        vm((R, HALF), BF16), vm((R, WIN), BF16), vm((R, D), BF16), vm((T, C, D), BF16), vm((T, TOK), jnp.int32),
        vm((2 * TOK, D), BF16), vm((n_dev * TOK, D), BF16), vm((2 * TOK, HALF), BF16),
        vm((C * T, D), F32), vm((C * T, D), BF16), vm((C * T, D), BF16),
        vm((WIN, R * T), BF16), vm((R * T, WIN), BF16),
        vm((N_CHIP * TOK, R * T), BF16), vm((N_CHIP * TOK, WIN), F32),
        vm((TOK, D), F32), vm((TOK, D), F32), vm((TOK, D), F32),
        vm((TOK, 128), BF16), vm((N_CHIP * TOK, 128), BF16),
        vm((4, T * TOK, D), BF16), vm((N_CHIP * T * TOK, WIN), BF16), vm((N_CHIP * T * TOK, R * T), BF16),
        vm((N_CHIP, TOK, R * T), F32), vm((N_CHIP, TOK, R * T), F32),
        vm((TOK, R * T), BF16), vm((n_dev * TOK, R * T), BF16),
        vm((R * T, WIN), F32), vm((R * T, OWIN), F32),
        vm((1, 128), F32), vm((n_dev, 1, 128), F32), vm((R * T, DP), F32),
        dma((16,)), dma((N_CHIP,)), dma((N_CHIP,)), dma, dma, dma((4,)), dma((4,)),
        dma((N_CHIP,)), dma((N_CHIP,)), dma((N_CHIP,)), dma((N_CHIP,)), dma, dma,
        dma((n_dev,)), dma((n_dev,)), dma((n_dev,)), dma((n_dev,)), dma, dma,
    ]

    def device_step(tokens, labels, w_one, w_two, adapter_a, adapter_b, task_heads):
        out_shapes = ((1, T), (R, D // n_dev), (R, FF // n_dev))
        call = pl.pallas_call(
            kernel,
            out_shape=tuple(pltpu.VMEM(s, F32) for s in out_shapes),
            in_specs=[pl.BlockSpec(memory_space=pltpu.HBM)] * 7,
            out_specs=tuple([pl.BlockSpec(memory_space=pltpu.VMEM)] * 3),
            scratch_shapes=scratch,
            compiler_params=pltpu.CompilerParams(
                collective_id=0, has_side_effects=True, vmem_limit_bytes=60 * 1024 * 1024
            ),
            name="min_norm",
        )
        put = pl.pallas_call(
            put_kernel,
            out_shape=tuple(jax.ShapeDtypeStruct(s, F32) for s in out_shapes),
            in_specs=[pl.BlockSpec(memory_space=pltpu.VMEM)] * 3,
            out_specs=tuple([pl.BlockSpec(memory_space=pltpu.HBM)] * 3),
            scratch_shapes=[dma((3,))],
            compiler_params=pltpu.CompilerParams(vmem_limit_bytes=1024 * 1024),
            name="put",
        )
        results = call(
            tokens, labels, w_one, w_two.T, adapter_a.T, adapter_b, task_heads.transpose(0, 2, 1)
        )
        alpha, ga_t, gb = put(*results)
        return alpha.reshape(T), ga_t.T, gb

    return jax.shard_map(
        device_step,
        mesh=mesh,
        in_specs=(P("data", None), P(None, "data"), P(), P(), P(), P(), P()),
        out_specs=(P(), P("data", None), P(None, "data")),
        check_vma=False,
    )
```

```python
import jax
import jax.numpy as jnp
from jax import lax
from jax.experimental import pallas as pl
from jax.experimental.pallas import tpu as pltpu
from jax.sharding import PartitionSpec as P

EG_STEPS = 20
_cur = [None]


def ph(name):
    if _cur[0] is not None:
        _cur[0].__exit__(None, None, None)
    _cur[0] = jax.named_scope(name) if name else None
    if name:
        _cur[0].__enter__()
F32 = jnp.float32
BF16 = jnp.bfloat16
MESH = pl.DeviceIdType.MESH

N_CHIP, N_CORE = 8, 2
TOK = 32
D, FF, R, T, C = 1600, 6400, 16, 8, 2
DP = 1664
HALF = FF // N_CORE
BLK = FF // N_CHIP
OWN = BLK // N_CORE
WIN = 896
OWIN = 512
W1_CHUNKS = ((0, 1536), (1536, 1664))
W2_CHUNKS = ((0, 1024), (1024, 576))
NEAR, FAR = (0, 1, 2, 4), (3, 5, 6, 7)
BLOCKS = ((0,), (1, 2), (3, 5, 6, 7), (4,))
GELU_C = 0.7978845608028654
N_TILE = 256


def nt(a, b):
    return lax.dot_general(a, b, (((1,), (1,)), ((), ())), preferred_element_type=F32)


def tn(a, b):
    return lax.dot_general(a, b, (((0,), (0,)), ((), ())), preferred_element_type=F32)


def nn(a, b):
    return jnp.dot(a, b, preferred_element_type=F32)


def gelu(p):
    th = jnp.tanh(GELU_C * (p + 0.044715 * (p * p * p)))
    return p * (0.5 * (1.0 + th))


def gelu_slope(p):
    p2 = p * p
    th = jnp.tanh(GELU_C * (p + 0.044715 * (p2 * p)))
    return 0.5 * (1.0 + th) + (0.5 * p * (1.0 - th * th)) * (GELU_C * (1.0 + 0.134145 * p2))


def iota(shape, dim):
    return lax.broadcasted_iota(jnp.int32, shape, dim)


def gram_parts(blocks):
    acc = [None] * 5
    for v in blocks:
        for k in range(5):
            w = v * (v if k == 0 else pltpu.roll(v, k, 0))
            w = sum(w[:, i : i + 128] for i in range(0, w.shape[1], 128))
            acc[k] = w if acc[k] is None else acc[k] + w
    return acc


def kernel(
    x_hbm, lab_hbm, w1_hbm, w2_hbm, at_hbm, bm_hbm, hd_hbm,
    alpha_out, ga_out, gb_out,
    w1h, w2h, w1w, w2w, bmh, bmw, at, hd, lab, xp, xall, hbuf, hs, ha, hb, bmt, bms, urep, g,
    zown, zsend, zrecv, eown, eall, dz, dp, ub, dsend, drecv, duown, duall, gb, gbrecv, mown, mall, ga,
    lsem, xs, xr, ps, pr, zs, zr, es, er, ds_, dr, bs, br, ns, nr, ms, mr, gs, gr,
):
    me = lax.axis_index("data")
    chip, core = me // N_CORE, me % N_CORE
    cx, cy, cz = chip % 2, (chip // 2) % 2, chip // 4
    mate = 1 - core

    def peer(m):
        px = 1 - cx if m & 1 else cx
        py = 1 - cy if m & 2 else cy
        pz = 1 - cz if m & 4 else cz
        return 4 * pz + 2 * py + px

    def rcopy(src, dst, ssem, rsem, chip_to, core_to):
        return pltpu.make_async_remote_copy(
            src_ref=src, dst_ref=dst, send_sem=ssem, recv_sem=rsem,
            device_id=(N_CORE * chip_to + core_to,), device_id_type=MESH,
        )

    n_sem = [0]

    def load(src, dst):
        c = pltpu.make_async_copy(src, dst, lsem.at[n_sem[0]])
        n_sem[0] += 1
        c.start()
        return c

    ph("prologue")
    half0 = pl.multiple_of(core * HALF, 128)
    tile0 = (BLK * chip) // 128
    win0 = pl.multiple_of(tile0 * 128, 128)
    off = BLK * chip - win0
    c_x = load(x_hbm, xp.at[pl.ds(0, TOK)])
    c_at = load(at_hbm, at)
    c_hd = load(hd_hbm, hd)
    c_lab = load(lab_hbm, lab)
    c_bmh = load(bm_hbm.at[:, pl.ds(half0, HALF)], bmh)
    c_bmw = load(bm_hbm.at[:, pl.ds(win0, WIN)], bmw)
    c_w1 = [load(w1_hbm.at[:, pl.ds(pl.multiple_of(half0 + a, 128), n)], w1h.at[:, pl.ds(a, n)]) for a, n in W1_CHUNKS]
    c_w2 = [load(w2_hbm.at[pl.ds(a, n), pl.ds(half0, HALF)], w2h.at[pl.ds(a, n)]) for a, n in W2_CHUNKS]
    c_w1w = load(w1_hbm.at[:, pl.ds(win0, WIN)], w1w.at[:, pl.ds(0, WIN)])
    c_w2w = load(w2_hbm.at[:, pl.ds(win0, WIN)], w2w)

    ph("barsig")
    barrier = pltpu.get_barrier_semaphore()
    for m in range(N_CHIP):
        for other in range(N_CORE):
            if m or other:
                pl.semaphore_signal(
                    barrier, inc=1, device_id=(N_CORE * peer(m) + (mate if other else core),), device_id_type=MESH
                )

    eown[...] = jnp.zeros_like(eown)
    row_of_r = (iota((R, R * T), 1) // T == iota((R, R * T), 0)).astype(F32).astype(BF16)
    c_hd.wait()
    for t in range(T):
        v = hd[t].astype(F32)
        for c in range(C):
            hs[pl.ds(c * T + t, 1), :] = v[c : c + 1]
    ha[...] = hs[...].astype(BF16)
    hb[...] = jnp.concatenate([hs[T:, :], hs[:T, :]], axis=0).astype(BF16)
    c_lab.wait()
    lab_f = lab[...].astype(F32)
    eye = (iota((TOK, TOK), 0) == iota((TOK, TOK), 1)).astype(F32).astype(BF16)
    lab_t = nt(eye, jnp.concatenate([lab_f, lab_f], axis=0).astype(BF16))
    onehot = (lab_t == (iota((TOK, C * T), 1) // T).astype(F32)).astype(F32)
    c_x.wait()
    my_row = pl.multiple_of(core * (N_CHIP * TOK) + chip * TOK, TOK)
    xall[pl.ds(my_row, TOK), :] = xp[pl.ds(0, TOK), :]

    ph("barwait")
    pl.semaphore_wait(barrier, N_CHIP * N_CORE - 1)

    ph("sends")
    k_xp = rcopy(xp.at[pl.ds(0, TOK)], xp.at[pl.ds(TOK, TOK)], ps, pr, chip, mate)
    k_xp.start()
    k_x = {}
    for m in (1, 2, 4, 7):
        k_x[m] = rcopy(xp.at[pl.ds(0, TOK)], xall.at[pl.ds(my_row, TOK)], xs.at[m], xr.at[m], peer(m), core)
        k_x[m].start()

    ph("prep2")
    c_at.wait()
    w1w[:, WIN:] = tn(at[...], row_of_r).astype(BF16)
    c_bmw.wait()
    colw = iota((R, WIN), 1)
    bm_f = jnp.where((colw >= off) & (colw < off + BLK), bmw[...].astype(F32), 0.0)
    bmt[...] = tn(bm_f.astype(BF16), row_of_r).astype(BF16)
    first_of_r = (T * iota((R, R * T), 0) == iota((R, R * T), 1)).astype(F32).astype(BF16)
    bms[...] = tn(first_of_r, bmw[...]).astype(BF16)

    ph("w_xp")
    k_xp.wait_recv()
    ph("u2")
    x2 = xp[...]
    u2 = nt(x2, at[...]).astype(BF16)
    c_bmh.wait()
    for (a, n), cp in zip(W1_CHUNKS, c_w1):
        ph("w_w1")
        cp.wait()
        ph("p1")
        for i in range(a, a + n, N_TILE):
            j = min(i + N_TILE, a + n)
            pre = nn(x2, w1h[:, i:j]) + nn(u2, bmh[:, i:j])
            hbuf[:, i:j] = gelu(pre).astype(BF16)
    k_z = []
    grp_row = pl.multiple_of(core * (N_CHIP * TOK), N_CHIP * TOK)

    def relay():
        ph("w_xnear")
        for got in (1, 2, 4):
            k_x[got].wait_recv()
        ph("relay")
        for got, to in ((1, 2), (2, 4), (4, 1)):
            rows = xall.at[pl.ds(pl.multiple_of(grp_row + peer(got) * TOK, TOK), TOK)]
            k_x[got + to] = rcopy(rows, rows, xs.at[got + to], xr.at[got + to], peer(to), core)
            k_x[got + to].start()

    for i, ((a, n), cp) in enumerate(zip(W2_CHUNKS, c_w2)):
        ph("w_w2")
        cp.wait()
        ph("p2")
        for j in range(a, a + n, N_TILE):
            z = nt(hbuf[...], w2h[j : min(j + N_TILE, a + n), :])
            zown[:, j : min(j + N_TILE, a + n)] = z[:TOK]
            zsend[:, j : min(j + N_TILE, a + n)] = z[TOK:]
        k_z.append(rcopy(zsend.at[:, pl.ds(a, n)], zrecv.at[:, pl.ds(a, n)], zs.at[i], zr.at[i], chip, mate))
        k_z[-1].start()
        if i == 0:
            relay()

    ph("w_w1w")
    c_w1w.wait()

    def slopes(which, base):
        ph("w_x")
        for m in which:
            if m in FAR:
                k_x[m].wait_recv()
        ph("slp")
        xc = jnp.concatenate(
            [xall[pl.ds(pl.multiple_of(grp_row + peer(m) * TOK, TOK), TOK), :] for m in which], axis=0
        )
        n_row = len(which) * TOK
        last = WIN - WIN % N_TILE
        pre = nn(xc, w1w[:, last:])
        ur = pre[:, WIN - last :].astype(BF16)
        urep[base : base + n_row, :] = ur
        pre = pre[:, : WIN - last] + nn(ur, bms[:, last:])
        g[base : base + n_row, last:] = gelu_slope(pre)
        for a in range(0, last, N_TILE):
            pre = nn(xc, w1w[:, a : a + N_TILE]) + nn(ur, bms[:, a : a + N_TILE])
            g[base : base + n_row, a : a + N_TILE] = gelu_slope(pre)

    slopes(NEAR, 0)
    ph("w_z")
    for k in k_z:
        k.wait_recv()
    ph("logits")
    xf = xp[pl.ds(0, TOK), :].astype(F32)
    zb = (xf + (zown[...] + zrecv[...])).astype(BF16)
    la, lb = nt(zb, ha[...]), nt(zb, hb[...])
    top = jnp.maximum(la, lb)
    ea, eb = jnp.exp(la - top), jnp.exp(lb - top)
    err = (ea / (ea + eb) - onehot).astype(BF16)
    eown[:, : C * T] = err
    my_slot = pl.multiple_of(chip * TOK, TOK)
    eall[pl.ds(my_slot, TOK), :] = eown[...]
    ph("esend")
    k_e = {}
    for m in (1, 2, 4, 3, 5, 6, 7):
        k_e[m] = rcopy(eown, eall.at[pl.ds(my_slot, TOK)], es.at[m], er.at[m], peer(m), core)
        k_e[m].start()

    ph("w_w2w")
    c_w2w.wait()
    lane_t = iota((TOK, R * T), 1) % T
    rel = {m: i * TOK for i, m in enumerate(NEAR + FAR)}
    k_d = {}

    def backward(block):
        ph("w_e")
        for m in block:
            if m:
                k_e[m].wait_recv()
        ph("back")
        dus = {}
        for m in block:
            r0 = rel[m] * T
            e = eall[pl.ds(pl.multiple_of(peer(m) * TOK, TOK), TOK), :].astype(F32)
            for t in range(T):
                dz[rel[m] // TOK % 4, t * TOK : (t + 1) * TOK, :] = (
                    e[:, t : t + 1] * hs[pl.ds(t, 1), :] + e[:, T + t : T + t + 1] * hs[pl.ds(T + t, 1), :]
                ).astype(BF16)
            for a in range(0, WIN, N_TILE):
                n = min(N_TILE, WIN - a)
                dh = nn(dz[rel[m] // TOK % 4], w2w[:, a : a + n]).reshape(T, TOK, n)
                slope = g[rel[m] : rel[m] + TOK, a : a + n]
                dp[r0 : r0 + T * TOK, a : a + n] = (dh * slope[None]).astype(BF16).reshape(T * TOK, n)
            du = nn(dp[r0 : r0 + T * TOK, :], bmt[...])
            dus[m] = sum(jnp.where(lane_t == t, du[t * TOK : (t + 1) * TOK], 0.0) for t in range(T))
            if m:
                dsend[m] = dus[m]
            ur = urep[rel[m] : rel[m] + TOK, :].astype(F32)
            for t in range(T):
                ub[r0 + t * TOK : r0 + (t + 1) * TOK, :] = jnp.where(lane_t == t, ur, 0.0).astype(BF16)
        for m in block:
            if m:
                k_d[m] = rcopy(dsend.at[m], drecv.at[m], ds_.at[m], dr.at[m], peer(m), core)
                k_d[m].start()
        return dus

    du_own = backward(BLOCKS[0])[0]
    for block in BLOCKS[1:]:
        if block == FAR:
            slopes(FAR, len(NEAR) * TOK)
            k_g = rcopy(xall.at[pl.ds(grp_row, N_CHIP * TOK)], xall.at[pl.ds(grp_row, N_CHIP * TOK)], gs, gr, chip, mate)
            k_g.start()
        backward(block)
    ph("gb")
    for a in range(0, WIN, N_TILE):
        gb[:, a : min(a + N_TILE, WIN)] = tn(ub[...], dp[:, a : min(a + N_TILE, WIN)])

    ph("gbsend")
    ow0 = pl.multiple_of(core * (OWIN - 128), 128)
    mw0 = pl.multiple_of(mate * (OWIN - 128), 128)
    k_b = rcopy(gb.at[:, pl.ds(mw0, OWIN)], gbrecv, bs, br, chip, mate)
    k_b.start()
    ph("w_du")
    for m in range(1, N_CHIP):
        k_d[m].wait_recv()
        du_own = du_own + drecv[m]
    ph("duag")
    duown[...] = du_own.astype(BF16)
    duall[pl.ds(my_row, TOK), :] = duown[...]
    others = [(m, o) for m in (7, 6, 5, 3, 4, 2, 1, 0) for o in range(N_CORE) if m or o]
    k_n = []
    for i, (m, o) in enumerate(others):
        k_n.append(rcopy(duown, duall.at[pl.ds(my_row, TOK)], ns.at[i], nr.at[i], peer(m), mate if o else core))
        k_n[-1].start()

    ph("w_gb")
    k_b.wait_recv()
    ph("gramb")
    off_own = off + 16 * core
    colo = iota((R * T, OWIN), 1)
    shard = (gb[:, pl.ds(ow0, OWIN)] + gbrecv[...]) * (1.0 / (N_CHIP * N_CORE * TOK))
    shard = jnp.where((colo >= off_own) & (colo < off_own + OWN), shard, 0.0)
    gbrecv[...] = shard
    lane = iota((T, 128), 1)
    sub = iota((T, 128), 0)
    parts = gram_parts([gbrecv[r * T : (r + 1) * T, :] for r in range(R)])
    row = sum(
        jnp.where(lane == T * k + sub, jnp.sum(p, axis=1, keepdims=True), 0.0) for k, p in enumerate(parts)
    )
    mown[...] = jnp.sum(row, axis=0, keepdims=True)
    mall[me] = mown[...]
    k_m = []
    for i, (m, o) in enumerate(others):
        k_m.append(rcopy(mown, mall.at[me], ms.at[i], mr.at[i], peer(m), mate if o else core))
        k_m[-1].start()

    ph("w_g")
    k_g.wait_recv()
    ph("w_duag")
    for k in k_n:
        k.wait_recv()
    ph("ga")
    ga[:, :D] = tn(duall[...], xall[...]) * (1.0 / (N_CHIP * N_CORE * TOK))
    ga[:, D:] = jnp.zeros((R * T, DP - D), F32)
    parts = gram_parts([ga[r * T : (r + 1) * T, :] for r in range(R)])
    ph("w_m")
    for k in k_m:
        k.wait_recv()
    ph("msum")
    mb = jnp.broadcast_to(sum(mall[i] for i in range(N_CHIP * N_CORE)), (T, 128))
    col = [
        jnp.sum(p + jnp.where(lane == T * k + sub, mb, 0.0), axis=1, keepdims=True) + jnp.zeros((T, 128), F32)
        for k, p in enumerate(parts)
    ]
    scale = jnp.sum(col[0], axis=0, keepdims=True) / T
    col = [c / scale for c in col]
    col += [pltpu.roll(col[T - k], k, 0) for k in range(5, T)]

    def eg_step(_, w):
        grad = sum(col[k] * (w if k == 0 else pltpu.roll(w, k, 0)) for k in range(T))
        w = w * jnp.exp(-grad)
        return w / jnp.sum(w, axis=0, keepdims=True)

    ph("eg")
    w = lax.fori_loop(0, EG_STEPS, eg_step, jnp.full((T, 128), 1.0 / T, F32))
    ph("out")
    alpha_out[...] = jnp.sum(jnp.where(lane == sub, w, 0.0), axis=0, keepdims=True)[:, :T]

    wcol = w[:, 0:1]
    dstart = (D // (N_CHIP * N_CORE)) * me
    dtile = dstart // 128
    da0 = pl.multiple_of(dtile * 128, 128)
    comb_a = jnp.concatenate(
        [jnp.sum(ga[r * T : (r + 1) * T, pl.ds(da0, 256)] * wcol, axis=0, keepdims=True) for r in range(R)], axis=0
    )
    ga_out[...] = pltpu.roll(comb_a, 256 - (dstart - da0), 1)[:, : D // (N_CHIP * N_CORE)]
    comb_b = jnp.concatenate(
        [jnp.sum(gbrecv[r * T : (r + 1) * T, :] * wcol, axis=0, keepdims=True) for r in range(R)], axis=0
    )
    gb_out[...] = pltpu.roll(comb_b, OWIN - off_own, 1)[:, :OWN]

    ph("w_send")
    for k in [k_xp, k_g, k_b] + k_z + k_n + k_m + [k_x[m] for m in k_x] + [k_e[m] for m in k_e] + [k_d[m] for m in k_d]:
        k.wait_send()
    ph(None)


def put_kernel(alpha_in, ga_in, gb_in, alpha_out, ga_out, gb_out, sem):
    pairs = ((alpha_in, alpha_out), (ga_in, ga_out), (gb_in, gb_out))
    copies = [pltpu.make_async_copy(a, b, sem.at[i]) for i, (a, b) in enumerate(pairs)]
    for c in copies:
        c.start()
    for c in copies:
        c.wait()


def solution(mesh):
    n_dev = mesh.shape["data"]
    assert n_dev == N_CHIP * N_CORE
    vm = pltpu.VMEM
    dma = pltpu.SemaphoreType.DMA
    scratch = [
        vm((D, HALF), BF16), vm((D, HALF), BF16), vm((D, WIN + R * T), BF16), vm((D, WIN), BF16),
        vm((R, HALF), BF16), vm((R, WIN), BF16), vm((R, D), BF16), vm((T, C, D), BF16), vm((T, TOK), jnp.int32),
        vm((2 * TOK, D), BF16), vm((n_dev * TOK, D), BF16), vm((2 * TOK, HALF), BF16),
        vm((C * T, D), F32), vm((C * T, D), BF16), vm((C * T, D), BF16),
        vm((WIN, R * T), BF16), vm((R * T, WIN), BF16),
        vm((N_CHIP * TOK, R * T), BF16), vm((N_CHIP * TOK, WIN), F32),
        vm((TOK, D), F32), vm((TOK, D), F32), vm((TOK, D), F32),
        vm((TOK, 128), BF16), vm((N_CHIP * TOK, 128), BF16),
        vm((4, T * TOK, D), BF16), vm((N_CHIP * T * TOK, WIN), BF16), vm((N_CHIP * T * TOK, R * T), BF16),
        vm((N_CHIP, TOK, R * T), F32), vm((N_CHIP, TOK, R * T), F32),
        vm((TOK, R * T), BF16), vm((n_dev * TOK, R * T), BF16),
        vm((R * T, WIN), F32), vm((R * T, OWIN), F32),
        vm((1, 128), F32), vm((n_dev, 1, 128), F32), vm((R * T, DP), F32),
        dma((16,)), dma((N_CHIP,)), dma((N_CHIP,)), dma, dma, dma((4,)), dma((4,)),
        dma((N_CHIP,)), dma((N_CHIP,)), dma((N_CHIP,)), dma((N_CHIP,)), dma, dma,
        dma((n_dev,)), dma((n_dev,)), dma((n_dev,)), dma((n_dev,)), dma, dma,
    ]

    def device_step(tokens, labels, w_one, w_two, adapter_a, adapter_b, task_heads):
        out_shapes = ((1, T), (R, D // n_dev), (R, FF // n_dev))
        call = pl.pallas_call(
            kernel,
            out_shape=tuple(pltpu.VMEM(s, F32) for s in out_shapes),
            in_specs=[pl.BlockSpec(memory_space=pltpu.HBM)] * 7,
            out_specs=tuple([pl.BlockSpec(memory_space=pltpu.VMEM)] * 3),
            scratch_shapes=scratch,
            compiler_params=pltpu.CompilerParams(
                collective_id=0, has_side_effects=True, vmem_limit_bytes=60 * 1024 * 1024
            ),
            name="min_norm",
        )
        put = pl.pallas_call(
            put_kernel,
            out_shape=tuple(jax.ShapeDtypeStruct(s, F32) for s in out_shapes),
            in_specs=[pl.BlockSpec(memory_space=pltpu.VMEM)] * 3,
            out_specs=tuple([pl.BlockSpec(memory_space=pltpu.HBM)] * 3),
            scratch_shapes=[dma((3,))],
            compiler_params=pltpu.CompilerParams(vmem_limit_bytes=1024 * 1024),
            name="put",
        )
        results = call(
            tokens, labels, w_one, w_two.T, adapter_a.T, adapter_b, task_heads.transpose(0, 2, 1)
        )
        alpha, ga_t, gb = put(*results)
        return alpha.reshape(T), ga_t.T, gb

    return jax.shard_map(
        device_step,
        mesh=mesh,
        in_specs=(P("data", None), P(None, "data"), P(), P(), P(), P(), P()),
        out_specs=(P(), P("data", None), P(None, "data")),
        check_vma=False,
    )
```

```python
import jax
import jax.numpy as jnp
from jax import lax
from jax.experimental import pallas as pl
from jax.experimental.pallas import tpu as pltpu
from jax.sharding import PartitionSpec as P

EG_STEPS = 20
_cur = [None]


def ph(name):
    if _cur[0] is not None:
        _cur[0].__exit__(None, None, None)
    _cur[0] = jax.named_scope(name) if name else None
    if name:
        _cur[0].__enter__()
F32 = jnp.float32
BF16 = jnp.bfloat16
MESH = pl.DeviceIdType.MESH

N_CHIP, N_CORE = 8, 2
TOK = 32
D, FF, R, T, C = 1600, 6400, 16, 8, 2
DP = 1664
HALF = FF // N_CORE
BLK = FF // N_CHIP
OWN = BLK // N_CORE
WIN = 896
OWIN = 512
W1_CHUNKS = ((0, 1536), (1536, 1664))
W2_CHUNKS = ((0, 512), (512, 512), (1024, 576))
NEAR, FAR = (0, 1, 2, 4), (3, 5, 6, 7)
BLOCKS = ((1, 2), (3, 5, 6, 7), (4,), (0,))
GELU_C = 0.7978845608028654
N_TILE = 256


def nt(a, b):
    return lax.dot_general(a, b, (((1,), (1,)), ((), ())), preferred_element_type=F32)


def tn(a, b):
    return lax.dot_general(a, b, (((0,), (0,)), ((), ())), preferred_element_type=F32)


def nn(a, b):
    return jnp.dot(a, b, preferred_element_type=F32)


def gelu(p):
    th = jnp.tanh(GELU_C * (p + 0.044715 * (p * p * p)))
    return p * (0.5 * (1.0 + th))


def gelu_slope(p):
    p2 = p * p
    th = jnp.tanh(GELU_C * (p + 0.044715 * (p2 * p)))
    return 0.5 * (1.0 + th) + (0.5 * p * (1.0 - th * th)) * (GELU_C * (1.0 + 0.134145 * p2))


def iota(shape, dim):
    return lax.broadcasted_iota(jnp.int32, shape, dim)


def gram_parts(blocks):
    acc = [None] * 5
    for v in blocks:
        for k in range(5):
            w = v * (v if k == 0 else pltpu.roll(v, k, 0))
            w = sum(w[:, i : i + 128] for i in range(0, w.shape[1], 128))
            acc[k] = w if acc[k] is None else acc[k] + w
    return acc


def kernel(
    x_hbm, lab_hbm, w1_hbm, w2_hbm, at_hbm, bm_hbm, hd_hbm,
    alpha_out, ga_out, gb_out,
    w1h, w2h, w1w, w2w, bmh, bmw, at, hd, lab, xp, xall, hbuf, hs, ha, hb, bmt, bms, urep, g,
    zown, zsend, zrecv, eown, eall, dz, dp, ub, dsend, drecv, duown, duall, gb, gbrecv, mown, mall, ga,
    lsem, xs, xr, ps, pr, zs, zr, es, er, ds_, dr, bs, br, ns, nr, ms, mr, gs, gr,
):
    me = lax.axis_index("data")
    chip, core = me // N_CORE, me % N_CORE
    cx, cy, cz = chip % 2, (chip // 2) % 2, chip // 4
    mate = 1 - core

    def peer(m):
        px = 1 - cx if m & 1 else cx
        py = 1 - cy if m & 2 else cy
        pz = 1 - cz if m & 4 else cz
        return 4 * pz + 2 * py + px

    def rcopy(src, dst, ssem, rsem, chip_to, core_to):
        return pltpu.make_async_remote_copy(
            src_ref=src, dst_ref=dst, send_sem=ssem, recv_sem=rsem,
            device_id=(N_CORE * chip_to + core_to,), device_id_type=MESH,
        )

    n_sem = [0]

    def load(src, dst):
        c = pltpu.make_async_copy(src, dst, lsem.at[n_sem[0]])
        n_sem[0] += 1
        c.start()
        return c

    ph("prologue")
    half0 = pl.multiple_of(core * HALF, 128)
    tile0 = (BLK * chip) // 128
    win0 = pl.multiple_of(tile0 * 128, 128)
    off = BLK * chip - win0
    c_x = load(x_hbm, xp.at[pl.ds(0, TOK)])
    c_at = load(at_hbm, at)
    c_hd = load(hd_hbm, hd)
    c_lab = load(lab_hbm, lab)
    c_bmh = load(bm_hbm.at[:, pl.ds(half0, HALF)], bmh)
    c_bmw = load(bm_hbm.at[:, pl.ds(win0, WIN)], bmw)
    c_w1 = [load(w1_hbm.at[:, pl.ds(pl.multiple_of(half0 + a, 128), n)], w1h.at[:, pl.ds(a, n)]) for a, n in W1_CHUNKS]
    c_w2 = [load(w2_hbm.at[pl.ds(a, n), pl.ds(half0, HALF)], w2h.at[pl.ds(a, n)]) for a, n in W2_CHUNKS]
    c_w1w = load(w1_hbm.at[:, pl.ds(win0, WIN)], w1w.at[:, pl.ds(0, WIN)])
    c_w2w = load(w2_hbm.at[:, pl.ds(win0, WIN)], w2w)

    ph("barsig")
    barrier = pltpu.get_barrier_semaphore()
    for m in range(N_CHIP):
        for other in range(N_CORE):
            if m or other:
                pl.semaphore_signal(
                    barrier, inc=1, device_id=(N_CORE * peer(m) + (mate if other else core),), device_id_type=MESH
                )

    eown[...] = jnp.zeros_like(eown)
    row_of_r = (iota((R, R * T), 1) // T == iota((R, R * T), 0)).astype(F32).astype(BF16)
    c_hd.wait()
    for t in range(T):
        v = hd[t].astype(F32)
        for c in range(C):
            hs[pl.ds(c * T + t, 1), :] = v[c : c + 1]
    ha[...] = hs[...].astype(BF16)
    hb[...] = jnp.concatenate([hs[T:, :], hs[:T, :]], axis=0).astype(BF16)
    c_lab.wait()
    lab_f = lab[...].astype(F32)
    eye = (iota((TOK, TOK), 0) == iota((TOK, TOK), 1)).astype(F32).astype(BF16)
    lab_t = nt(eye, jnp.concatenate([lab_f, lab_f], axis=0).astype(BF16))
    onehot = (lab_t == (iota((TOK, C * T), 1) // T).astype(F32)).astype(F32)
    c_x.wait()
    my_row = pl.multiple_of(core * (N_CHIP * TOK) + chip * TOK, TOK)
    xall[pl.ds(my_row, TOK), :] = xp[pl.ds(0, TOK), :]

    ph("barwait")
    pl.semaphore_wait(barrier, N_CHIP * N_CORE - 1)

    ph("sends")
    k_xp = rcopy(xp.at[pl.ds(0, TOK)], xp.at[pl.ds(TOK, TOK)], ps, pr, chip, mate)
    k_xp.start()
    k_x = {}
    for m in (1, 2, 4, 7):
        k_x[m] = rcopy(xp.at[pl.ds(0, TOK)], xall.at[pl.ds(my_row, TOK)], xs.at[m], xr.at[m], peer(m), core)
        k_x[m].start()

    ph("prep2")
    c_at.wait()
    w1w[:, WIN:] = tn(at[...], row_of_r).astype(BF16)
    c_bmw.wait()
    colw = iota((R, WIN), 1)
    bm_f = jnp.where((colw >= off) & (colw < off + BLK), bmw[...].astype(F32), 0.0)
    bmt[...] = tn(bm_f.astype(BF16), row_of_r).astype(BF16)
    first_of_r = (T * iota((R, R * T), 0) == iota((R, R * T), 1)).astype(F32).astype(BF16)
    bms[...] = tn(first_of_r, bmw[...]).astype(BF16)

    ph("w_xp")
    k_xp.wait_recv()
    ph("u2")
    x2 = xp[...]
    u2 = nt(x2, at[...]).astype(BF16)
    c_bmh.wait()
    for (a, n), cp in zip(W1_CHUNKS, c_w1):
        ph("w_w1")
        cp.wait()
        ph("p1")
        for i in range(a, a + n, N_TILE):
            j = min(i + N_TILE, a + n)
            pre = nn(x2, w1h[:, i:j]) + nn(u2, bmh[:, i:j])
            hbuf[:, i:j] = gelu(pre).astype(BF16)
    k_z = []
    grp_row = pl.multiple_of(core * (N_CHIP * TOK), N_CHIP * TOK)

    def relay():
        ph("w_xnear")
        for got in (1, 2, 4):
            k_x[got].wait_recv()
        ph("relay")
        for got, to in ((1, 2), (2, 4), (4, 1)):
            rows = xall.at[pl.ds(pl.multiple_of(grp_row + peer(got) * TOK, TOK), TOK)]
            k_x[got + to] = rcopy(rows, rows, xs.at[got + to], xr.at[got + to], peer(to), core)
            k_x[got + to].start()

    for i, ((a, n), cp) in enumerate(zip(W2_CHUNKS, c_w2)):
        ph("w_w2")
        cp.wait()
        ph("p2")
        for j in range(a, a + n, N_TILE):
            z = nt(hbuf[...], w2h[j : min(j + N_TILE, a + n), :])
            zown[:, j : min(j + N_TILE, a + n)] = z[:TOK]
            zsend[:, j : min(j + N_TILE, a + n)] = z[TOK:]
        k_z.append(rcopy(zsend.at[:, pl.ds(a, n)], zrecv.at[:, pl.ds(a, n)], zs.at[i], zr.at[i], chip, mate))
        k_z[-1].start()
        if i == 1:
            relay()

    ph("w_w1w")
    c_w1w.wait()

    def slopes(which, base):
        ph("w_x")
        for m in which:
            if m in FAR:
                k_x[m].wait_recv()
        ph("slp")
        xc = jnp.concatenate(
            [xall[pl.ds(pl.multiple_of(grp_row + peer(m) * TOK, TOK), TOK), :] for m in which], axis=0
        )
        n_row = len(which) * TOK
        last = WIN - WIN % N_TILE
        pre = nn(xc, w1w[:, last:])
        ur = pre[:, WIN - last :].astype(BF16)
        urep[base : base + n_row, :] = ur
        pre = pre[:, : WIN - last] + nn(ur, bms[:, last:])
        g[base : base + n_row, last:] = gelu_slope(pre)
        for a in range(0, last, N_TILE):
            pre = nn(xc, w1w[:, a : a + N_TILE]) + nn(ur, bms[:, a : a + N_TILE])
            g[base : base + n_row, a : a + N_TILE] = gelu_slope(pre)

    slopes(NEAR, 0)
    ph("w_z")
    for k in k_z:
        k.wait_recv()
    ph("logits")
    xf = xp[pl.ds(0, TOK), :].astype(F32)
    zb = (xf + (zown[...] + zrecv[...])).astype(BF16)
    la, lb = nt(zb, ha[...]), nt(zb, hb[...])
    top = jnp.maximum(la, lb)
    ea, eb = jnp.exp(la - top), jnp.exp(lb - top)
    err = (ea / (ea + eb) - onehot).astype(BF16)
    eown[:, : C * T] = err
    my_slot = pl.multiple_of(chip * TOK, TOK)
    eall[pl.ds(my_slot, TOK), :] = eown[...]
    ph("esend")
    k_e = {}
    for m in (1, 2, 4, 3, 5, 6, 7):
        k_e[m] = rcopy(eown, eall.at[pl.ds(my_slot, TOK)], es.at[m], er.at[m], peer(m), core)
        k_e[m].start()

    ph("w_w2w")
    c_w2w.wait()
    lane_t = iota((TOK, R * T), 1) % T
    rel = {m: i * TOK for i, m in enumerate(NEAR + FAR)}
    k_d = {}

    def backward(block):
        ph("w_e")
        for m in block:
            if m:
                k_e[m].wait_recv()
        ph("back")
        dus = {}
        for m in block:
            r0 = rel[m] * T
            e = eall[pl.ds(pl.multiple_of(peer(m) * TOK, TOK), TOK), :].astype(F32)
            for t in range(T):
                dz[rel[m] // TOK % 4, t * TOK : (t + 1) * TOK, :] = (
                    e[:, t : t + 1] * hs[pl.ds(t, 1), :] + e[:, T + t : T + t + 1] * hs[pl.ds(T + t, 1), :]
                ).astype(BF16)
            for a in range(0, WIN, N_TILE):
                n = min(N_TILE, WIN - a)
                dh = nn(dz[rel[m] // TOK % 4], w2w[:, a : a + n]).reshape(T, TOK, n)
                slope = g[rel[m] : rel[m] + TOK, a : a + n]
                dp[r0 : r0 + T * TOK, a : a + n] = (dh * slope[None]).astype(BF16).reshape(T * TOK, n)
            du = nn(dp[r0 : r0 + T * TOK, :], bmt[...])
            dus[m] = sum(jnp.where(lane_t == t, du[t * TOK : (t + 1) * TOK], 0.0) for t in range(T))
            if m:
                dsend[m] = dus[m]
            ur = urep[rel[m] : rel[m] + TOK, :].astype(F32)
            for t in range(T):
                ub[r0 + t * TOK : r0 + (t + 1) * TOK, :] = jnp.where(lane_t == t, ur, 0.0).astype(BF16)
        for m in block:
            if m:
                k_d[m] = rcopy(dsend.at[m], drecv.at[m], ds_.at[m], dr.at[m], peer(m), core)
                k_d[m].start()
        return dus

    slopes(FAR, len(NEAR) * TOK)
    k_g = rcopy(xall.at[pl.ds(grp_row, N_CHIP * TOK)], xall.at[pl.ds(grp_row, N_CHIP * TOK)], gs, gr, chip, mate)
    k_g.start()
    for block in BLOCKS[:-1]:
        backward(block)
    du_own = backward(BLOCKS[-1])[0]
    ph("gb")
    for a in range(0, WIN, N_TILE):
        gb[:, a : min(a + N_TILE, WIN)] = tn(ub[...], dp[:, a : min(a + N_TILE, WIN)])

    ph("gbsend")
    ow0 = pl.multiple_of(core * (OWIN - 128), 128)
    mw0 = pl.multiple_of(mate * (OWIN - 128), 128)
    k_b = rcopy(gb.at[:, pl.ds(mw0, OWIN)], gbrecv, bs, br, chip, mate)
    k_b.start()
    ph("w_du")
    for m in range(1, N_CHIP):
        k_d[m].wait_recv()
        du_own = du_own + drecv[m]
    ph("duag")
    duown[...] = du_own.astype(BF16)
    duall[pl.ds(my_row, TOK), :] = duown[...]
    others = [(m, o) for m in (7, 6, 5, 3, 4, 2, 1, 0) for o in range(N_CORE) if m or o]
    k_n = []
    for i, (m, o) in enumerate(others):
        k_n.append(rcopy(duown, duall.at[pl.ds(my_row, TOK)], ns.at[i], nr.at[i], peer(m), mate if o else core))
        k_n[-1].start()

    ph("w_gb")
    k_b.wait_recv()
    ph("gramb")
    off_own = off + 16 * core
    colo = iota((R * T, OWIN), 1)
    shard = (gb[:, pl.ds(ow0, OWIN)] + gbrecv[...]) * (1.0 / (N_CHIP * N_CORE * TOK))
    shard = jnp.where((colo >= off_own) & (colo < off_own + OWN), shard, 0.0)
    gbrecv[...] = shard
    lane = iota((T, 128), 1)
    sub = iota((T, 128), 0)
    parts = gram_parts([gbrecv[r * T : (r + 1) * T, :] for r in range(R)])
    row = sum(
        jnp.where(lane == T * k + sub, jnp.sum(p, axis=1, keepdims=True), 0.0) for k, p in enumerate(parts)
    )
    mown[...] = jnp.sum(row, axis=0, keepdims=True)
    mall[me] = mown[...]
    k_m = []
    for i, (m, o) in enumerate(others):
        k_m.append(rcopy(mown, mall.at[me], ms.at[i], mr.at[i], peer(m), mate if o else core))
        k_m[-1].start()

    ph("w_g")
    k_g.wait_recv()
    ph("w_duag")
    for k in k_n:
        k.wait_recv()
    ph("ga")
    ga[:, :D] = tn(duall[...], xall[...]) * (1.0 / (N_CHIP * N_CORE * TOK))
    ga[:, D:] = jnp.zeros((R * T, DP - D), F32)
    parts = gram_parts([ga[r * T : (r + 1) * T, :] for r in range(R)])
    ph("w_m")
    for k in k_m:
        k.wait_recv()
    ph("msum")
    mb = jnp.broadcast_to(sum(mall[i] for i in range(N_CHIP * N_CORE)), (T, 128))
    col = [
        jnp.sum(p + jnp.where(lane == T * k + sub, mb, 0.0), axis=1, keepdims=True) + jnp.zeros((T, 128), F32)
        for k, p in enumerate(parts)
    ]
    scale = jnp.sum(col[0], axis=0, keepdims=True) / T
    col = [c / scale for c in col]
    col += [pltpu.roll(col[T - k], k, 0) for k in range(5, T)]

    def eg_step(_, w):
        grad = sum(col[k] * (w if k == 0 else pltpu.roll(w, k, 0)) for k in range(T))
        w = w * jnp.exp(-grad)
        return w / jnp.sum(w, axis=0, keepdims=True)

    ph("eg")
    w = lax.fori_loop(0, EG_STEPS, eg_step, jnp.full((T, 128), 1.0 / T, F32))
    ph("out")
    alpha_out[...] = jnp.sum(jnp.where(lane == sub, w, 0.0), axis=0, keepdims=True)[:, :T]

    wcol = w[:, 0:1]
    dstart = (D // (N_CHIP * N_CORE)) * me
    dtile = dstart // 128
    da0 = pl.multiple_of(dtile * 128, 128)
    comb_a = jnp.concatenate(
        [jnp.sum(ga[r * T : (r + 1) * T, pl.ds(da0, 256)] * wcol, axis=0, keepdims=True) for r in range(R)], axis=0
    )
    ga_out[...] = pltpu.roll(comb_a, 256 - (dstart - da0), 1)[:, : D // (N_CHIP * N_CORE)]
    comb_b = jnp.concatenate(
        [jnp.sum(gbrecv[r * T : (r + 1) * T, :] * wcol, axis=0, keepdims=True) for r in range(R)], axis=0
    )
    gb_out[...] = pltpu.roll(comb_b, OWIN - off_own, 1)[:, :OWN]

    ph("w_send")
    for k in [k_xp, k_g, k_b] + k_z + k_n + k_m + [k_x[m] for m in k_x] + [k_e[m] for m in k_e] + [k_d[m] for m in k_d]:
        k.wait_send()
    ph(None)


def put_kernel(alpha_in, ga_in, gb_in, alpha_out, ga_out, gb_out, sem):
    pairs = ((alpha_in, alpha_out), (ga_in, ga_out), (gb_in, gb_out))
    copies = [pltpu.make_async_copy(a, b, sem.at[i]) for i, (a, b) in enumerate(pairs)]
    for c in copies:
        c.start()
    for c in copies:
        c.wait()


def solution(mesh):
    n_dev = mesh.shape["data"]
    assert n_dev == N_CHIP * N_CORE
    vm = pltpu.VMEM
    dma = pltpu.SemaphoreType.DMA
    scratch = [
        vm((D, HALF), BF16), vm((D, HALF), BF16), vm((D, WIN + R * T), BF16), vm((D, WIN), BF16),
        vm((R, HALF), BF16), vm((R, WIN), BF16), vm((R, D), BF16), vm((T, C, D), BF16), vm((T, TOK), jnp.int32),
        vm((2 * TOK, D), BF16), vm((n_dev * TOK, D), BF16), vm((2 * TOK, HALF), BF16),
        vm((C * T, D), F32), vm((C * T, D), BF16), vm((C * T, D), BF16),
        vm((WIN, R * T), BF16), vm((R * T, WIN), BF16),
        vm((N_CHIP * TOK, R * T), BF16), vm((N_CHIP * TOK, WIN), F32),
        vm((TOK, D), F32), vm((TOK, D), F32), vm((TOK, D), F32),
        vm((TOK, 128), BF16), vm((N_CHIP * TOK, 128), BF16),
        vm((4, T * TOK, D), BF16), vm((N_CHIP * T * TOK, WIN), BF16), vm((N_CHIP * T * TOK, R * T), BF16),
        vm((N_CHIP, TOK, R * T), F32), vm((N_CHIP, TOK, R * T), F32),
        vm((TOK, R * T), BF16), vm((n_dev * TOK, R * T), BF16),
        vm((R * T, WIN), F32), vm((R * T, OWIN), F32),
        vm((1, 128), F32), vm((n_dev, 1, 128), F32), vm((R * T, DP), F32),
        dma((16,)), dma((N_CHIP,)), dma((N_CHIP,)), dma, dma, dma((4,)), dma((4,)),
        dma((N_CHIP,)), dma((N_CHIP,)), dma((N_CHIP,)), dma((N_CHIP,)), dma, dma,
        dma((n_dev,)), dma((n_dev,)), dma((n_dev,)), dma((n_dev,)), dma, dma,
    ]

    def device_step(tokens, labels, w_one, w_two, adapter_a, adapter_b, task_heads):
        out_shapes = ((1, T), (R, D // n_dev), (R, FF // n_dev))
        call = pl.pallas_call(
            kernel,
            out_shape=tuple(pltpu.VMEM(s, F32) for s in out_shapes),
            in_specs=[pl.BlockSpec(memory_space=pltpu.HBM)] * 7,
            out_specs=tuple([pl.BlockSpec(memory_space=pltpu.VMEM)] * 3),
            scratch_shapes=scratch,
            compiler_params=pltpu.CompilerParams(
                collective_id=0, has_side_effects=True, vmem_limit_bytes=60 * 1024 * 1024
            ),
            name="min_norm",
        )
        put = pl.pallas_call(
            put_kernel,
            out_shape=tuple(jax.ShapeDtypeStruct(s, F32) for s in out_shapes),
            in_specs=[pl.BlockSpec(memory_space=pltpu.VMEM)] * 3,
            out_specs=tuple([pl.BlockSpec(memory_space=pltpu.HBM)] * 3),
            scratch_shapes=[dma((3,))],
            compiler_params=pltpu.CompilerParams(vmem_limit_bytes=1024 * 1024),
            name="put",
        )
        results = call(
            tokens, labels, w_one, w_two.T, adapter_a.T, adapter_b, task_heads.transpose(0, 2, 1)
        )
        alpha, ga_t, gb = put(*results)
        return alpha.reshape(T), ga_t.T, gb

    return jax.shard_map(
        device_step,
        mesh=mesh,
        in_specs=(P("data", None), P(None, "data"), P(), P(), P(), P(), P()),
        out_specs=(P(), P("data", None), P(None, "data")),
        check_vma=False,
    )
```

```python
import jax
import jax.numpy as jnp
from jax import lax
from jax.experimental import pallas as pl
from jax.experimental.pallas import tpu as pltpu
from jax.sharding import PartitionSpec as P

EG_STEPS = 20
F32 = jnp.float32
BF16 = jnp.bfloat16
MESH = pl.DeviceIdType.MESH

N_CHIP, N_CORE = 8, 2
TOK = 32
D, FF, R, T, C = 1600, 6400, 16, 8, 2
DP = 1664
HALF = FF // N_CORE
BLK = FF // N_CHIP
OWN = BLK // N_CORE
WIN = 896
OWIN = 512
W1_CHUNKS = ((0, 1536), (1536, 1664))
W2_CHUNKS = ((0, 512), (512, 512), (1024, 576))
NEAR, FAR = (0, 1, 2, 4), (3, 5, 6, 7)
BLOCKS = ((1, 2), (3, 5, 6, 7), (4,), (0,))
GELU_C = 0.7978845608028654
N_TILE = 256


def nt(a, b):
    return lax.dot_general(a, b, (((1,), (1,)), ((), ())), preferred_element_type=F32)


def tn(a, b):
    return lax.dot_general(a, b, (((0,), (0,)), ((), ())), preferred_element_type=F32)


def nn(a, b):
    return jnp.dot(a, b, preferred_element_type=F32)


def gelu(p):
    th = jnp.tanh(GELU_C * (p + 0.044715 * (p * p * p)))
    return p * (0.5 * (1.0 + th))


def gelu_slope(p):
    p2 = p * p
    th = jnp.tanh(GELU_C * (p + 0.044715 * (p2 * p)))
    return 0.5 * (1.0 + th) + (0.5 * p * (1.0 - th * th)) * (GELU_C * (1.0 + 0.134145 * p2))


def iota(shape, dim):
    return lax.broadcasted_iota(jnp.int32, shape, dim)


def gram_parts(blocks):
    acc = [None] * 5
    for v in blocks:
        for k in range(5):
            w = v * (v if k == 0 else pltpu.roll(v, k, 0))
            w = sum(w[:, i : i + 128] for i in range(0, w.shape[1], 128))
            acc[k] = w if acc[k] is None else acc[k] + w
    return acc


def kernel(
    x_hbm, lab_hbm, w1_hbm, w2_hbm, at_hbm, bm_hbm, hd_hbm,
    alpha_out, ga_out, gb_out,
    w1h, w2h, w1w, w2w, bmh, bmw, at, hd, lab, xp, xall, hbuf, hs, ha, hb, bmt, bms, urep, g,
    zown, zsend, zrecv, eown, eall, dz, dp, ub, dsend, drecv, duown, duall, gb, gbrecv, mown, mall, ga,
    lsem, xs, xr, ps, pr, zs, zr, es, er, ds_, dr, bs, br, ns, nr, ms, mr, gs, gr,
):
    me = lax.axis_index("data")
    chip, core = me // N_CORE, me % N_CORE
    cx, cy, cz = chip % 2, (chip // 2) % 2, chip // 4
    mate = 1 - core

    def peer(m):
        px = 1 - cx if m & 1 else cx
        py = 1 - cy if m & 2 else cy
        pz = 1 - cz if m & 4 else cz
        return 4 * pz + 2 * py + px

    def rcopy(src, dst, ssem, rsem, chip_to, core_to):
        return pltpu.make_async_remote_copy(
            src_ref=src, dst_ref=dst, send_sem=ssem, recv_sem=rsem,
            device_id=(N_CORE * chip_to + core_to,), device_id_type=MESH,
        )

    n_sem = [0]

    def load(src, dst):
        c = pltpu.make_async_copy(src, dst, lsem.at[n_sem[0]])
        n_sem[0] += 1
        c.start()
        return c

    half0 = pl.multiple_of(core * HALF, 128)
    tile0 = (BLK * chip) // 128
    win0 = pl.multiple_of(tile0 * 128, 128)
    off = BLK * chip - win0
    c_x = load(x_hbm, xp.at[pl.ds(0, TOK)])
    c_at = load(at_hbm, at)
    c_hd = load(hd_hbm, hd)
    c_lab = load(lab_hbm, lab)
    c_bmh = load(bm_hbm.at[:, pl.ds(half0, HALF)], bmh)
    c_bmw = load(bm_hbm.at[:, pl.ds(win0, WIN)], bmw)
    c_w1 = [load(w1_hbm.at[:, pl.ds(pl.multiple_of(half0 + a, 128), n)], w1h.at[:, pl.ds(a, n)]) for a, n in W1_CHUNKS]
    c_w2 = [load(w2_hbm.at[pl.ds(a, n), pl.ds(half0, HALF)], w2h.at[pl.ds(a, n)]) for a, n in W2_CHUNKS]
    c_w1w = load(w1_hbm.at[:, pl.ds(win0, WIN)], w1w.at[:, pl.ds(0, WIN)])
    c_w2w = load(w2_hbm.at[:, pl.ds(win0, WIN)], w2w)

    barrier = pltpu.get_barrier_semaphore()
    for m in range(N_CHIP):
        for other in range(N_CORE):
            if m or other:
                pl.semaphore_signal(
                    barrier, inc=1, device_id=(N_CORE * peer(m) + (mate if other else core),), device_id_type=MESH
                )

    eown[...] = jnp.zeros_like(eown)
    row_of_r = (iota((R, R * T), 1) // T == iota((R, R * T), 0)).astype(F32).astype(BF16)
    c_hd.wait()
    for t in range(T):
        v = hd[t].astype(F32)
        for c in range(C):
            hs[pl.ds(c * T + t, 1), :] = v[c : c + 1]
    ha[...] = hs[...].astype(BF16)
    hb[...] = jnp.concatenate([hs[T:, :], hs[:T, :]], axis=0).astype(BF16)
    c_lab.wait()
    lab_f = lab[...].astype(F32)
    eye = (iota((TOK, TOK), 0) == iota((TOK, TOK), 1)).astype(F32).astype(BF16)
    lab_t = nt(eye, jnp.concatenate([lab_f, lab_f], axis=0).astype(BF16))
    onehot = (lab_t == (iota((TOK, C * T), 1) // T).astype(F32)).astype(F32)
    c_x.wait()
    my_row = pl.multiple_of(core * (N_CHIP * TOK) + chip * TOK, TOK)
    xall[pl.ds(my_row, TOK), :] = xp[pl.ds(0, TOK), :]

    pl.semaphore_wait(barrier, N_CHIP * N_CORE - 1)

    k_xp = rcopy(xp.at[pl.ds(0, TOK)], xp.at[pl.ds(TOK, TOK)], ps, pr, chip, mate)
    k_xp.start()
    k_x = {}
    for m in (1, 2, 4, 7):
        k_x[m] = rcopy(xp.at[pl.ds(0, TOK)], xall.at[pl.ds(my_row, TOK)], xs.at[m], xr.at[m], peer(m), core)
        k_x[m].start()

    c_at.wait()
    w1w[:, WIN:] = tn(at[...], row_of_r).astype(BF16)
    c_bmw.wait()
    colw = iota((R, WIN), 1)
    bm_f = jnp.where((colw >= off) & (colw < off + BLK), bmw[...].astype(F32), 0.0)
    bmt[...] = tn(bm_f.astype(BF16), row_of_r).astype(BF16)
    first_of_r = (T * iota((R, R * T), 0) == iota((R, R * T), 1)).astype(F32).astype(BF16)
    bms[...] = tn(first_of_r, bmw[...]).astype(BF16)

    k_xp.wait_recv()
    x2 = xp[...]
    u2 = nt(x2, at[...]).astype(BF16)
    c_bmh.wait()
    for (a, n), cp in zip(W1_CHUNKS, c_w1):
        cp.wait()
        for i in range(a, a + n, N_TILE):
            j = min(i + N_TILE, a + n)
            pre = nn(x2, w1h[:, i:j]) + nn(u2, bmh[:, i:j])
            hbuf[:, i:j] = gelu(pre).astype(BF16)
    k_z = []
    grp_row = pl.multiple_of(core * (N_CHIP * TOK), N_CHIP * TOK)

    def relay():
        for got in (1, 2, 4):
            k_x[got].wait_recv()
        for got, to in ((1, 2), (2, 4), (4, 1)):
            rows = xall.at[pl.ds(pl.multiple_of(grp_row + peer(got) * TOK, TOK), TOK)]
            k_x[got + to] = rcopy(rows, rows, xs.at[got + to], xr.at[got + to], peer(to), core)
            k_x[got + to].start()

    for i, ((a, n), cp) in enumerate(zip(W2_CHUNKS, c_w2)):
        cp.wait()
        for j in range(a, a + n, N_TILE):
            z = nt(hbuf[...], w2h[j : min(j + N_TILE, a + n), :])
            zown[:, j : min(j + N_TILE, a + n)] = z[:TOK]
            zsend[:, j : min(j + N_TILE, a + n)] = z[TOK:]
        k_z.append(rcopy(zsend.at[:, pl.ds(a, n)], zrecv.at[:, pl.ds(a, n)], zs.at[i], zr.at[i], chip, mate))
        k_z[-1].start()
        if i == 0:
            relay()

    c_w1w.wait()

    def slopes(which, base):
        for m in which:
            if m in FAR:
                k_x[m].wait_recv()
        xc = jnp.concatenate(
            [xall[pl.ds(pl.multiple_of(grp_row + peer(m) * TOK, TOK), TOK), :] for m in which], axis=0
        )
        n_row = len(which) * TOK
        last = WIN - WIN % N_TILE
        pre = nn(xc, w1w[:, last:])
        ur = pre[:, WIN - last :].astype(BF16)
        urep[base : base + n_row, :] = ur
        pre = pre[:, : WIN - last] + nn(ur, bms[:, last:])
        g[base : base + n_row, last:] = gelu_slope(pre)
        for a in range(0, last, N_TILE):
            pre = nn(xc, w1w[:, a : a + N_TILE]) + nn(ur, bms[:, a : a + N_TILE])
            g[base : base + n_row, a : a + N_TILE] = gelu_slope(pre)

    slopes(NEAR, 0)
    for k in k_z:
        k.wait_recv()
    xf = xp[pl.ds(0, TOK), :].astype(F32)
    zb = (xf + (zown[...] + zrecv[...])).astype(BF16)
    la, lb = nt(zb, ha[...]), nt(zb, hb[...])
    top = jnp.maximum(la, lb)
    ea, eb = jnp.exp(la - top), jnp.exp(lb - top)
    err = (ea / (ea + eb) - onehot).astype(BF16)
    eown[:, : C * T] = err
    my_slot = pl.multiple_of(chip * TOK, TOK)
    eall[pl.ds(my_slot, TOK), :] = eown[...]
    k_e = {}
    for m in (1, 2, 4, 3, 5, 6, 7):
        k_e[m] = rcopy(eown, eall.at[pl.ds(my_slot, TOK)], es.at[m], er.at[m], peer(m), core)
        k_e[m].start()

    c_w2w.wait()
    lane_t = iota((TOK, R * T), 1) % T
    rel = {m: i * TOK for i, m in enumerate(NEAR + FAR)}
    k_d = {}

    def backward(block):
        for m in block:
            if m:
                k_e[m].wait_recv()
        dus = {}
        for m in block:
            r0 = rel[m] * T
            e = eall[pl.ds(pl.multiple_of(peer(m) * TOK, TOK), TOK), :].astype(F32)
            for t in range(T):
                dz[rel[m] // TOK % 4, t * TOK : (t + 1) * TOK, :] = (
                    e[:, t : t + 1] * hs[pl.ds(t, 1), :] + e[:, T + t : T + t + 1] * hs[pl.ds(T + t, 1), :]
                ).astype(BF16)
            for a in range(0, WIN, N_TILE):
                n = min(N_TILE, WIN - a)
                dh = nn(dz[rel[m] // TOK % 4], w2w[:, a : a + n]).reshape(T, TOK, n)
                slope = g[rel[m] : rel[m] + TOK, a : a + n]
                dp[r0 : r0 + T * TOK, a : a + n] = (dh * slope[None]).astype(BF16).reshape(T * TOK, n)
            du = nn(dp[r0 : r0 + T * TOK, :], bmt[...])
            dus[m] = sum(jnp.where(lane_t == t, du[t * TOK : (t + 1) * TOK], 0.0) for t in range(T))
            if m:
                dsend[m] = dus[m]
            ur = urep[rel[m] : rel[m] + TOK, :].astype(F32)
            for t in range(T):
                ub[r0 + t * TOK : r0 + (t + 1) * TOK, :] = jnp.where(lane_t == t, ur, 0.0).astype(BF16)
        for m in block:
            if m:
                k_d[m] = rcopy(dsend.at[m], drecv.at[m], ds_.at[m], dr.at[m], peer(m), core)
                k_d[m].start()
        return dus

    slopes(FAR, len(NEAR) * TOK)
    k_g = rcopy(xall.at[pl.ds(grp_row, N_CHIP * TOK)], xall.at[pl.ds(grp_row, N_CHIP * TOK)], gs, gr, chip, mate)
    k_g.start()
    for block in BLOCKS[:-1]:
        backward(block)
    du_own = backward(BLOCKS[-1])[0]
    for a in range(0, WIN, N_TILE):
        gb[:, a : min(a + N_TILE, WIN)] = tn(ub[...], dp[:, a : min(a + N_TILE, WIN)])

    ow0 = pl.multiple_of(core * (OWIN - 128), 128)
    mw0 = pl.multiple_of(mate * (OWIN - 128), 128)
    k_b = rcopy(gb.at[:, pl.ds(mw0, OWIN)], gbrecv, bs, br, chip, mate)
    k_b.start()
    for m in range(1, N_CHIP):
        k_d[m].wait_recv()
        du_own = du_own + drecv[m]
    duown[...] = du_own.astype(BF16)
    duall[pl.ds(my_row, TOK), :] = duown[...]
    others = [(m, o) for m in (7, 6, 5, 3, 4, 2, 1, 0) for o in range(N_CORE) if m or o]
    k_n = []
    for i, (m, o) in enumerate(others):
        k_n.append(rcopy(duown, duall.at[pl.ds(my_row, TOK)], ns.at[i], nr.at[i], peer(m), mate if o else core))
        k_n[-1].start()

    k_b.wait_recv()
    off_own = off + 16 * core
    colo = iota((R * T, OWIN), 1)
    shard = (gb[:, pl.ds(ow0, OWIN)] + gbrecv[...]) * (1.0 / (N_CHIP * N_CORE * TOK))
    shard = jnp.where((colo >= off_own) & (colo < off_own + OWN), shard, 0.0)
    gbrecv[...] = shard
    lane = iota((T, 128), 1)
    sub = iota((T, 128), 0)
    parts = gram_parts([gbrecv[r * T : (r + 1) * T, :] for r in range(R)])
    row = sum(
        jnp.where(lane == T * k + sub, jnp.sum(p, axis=1, keepdims=True), 0.0) for k, p in enumerate(parts)
    )
    mown[...] = jnp.sum(row, axis=0, keepdims=True)
    mall[me] = mown[...]
    k_m = []
    for i, (m, o) in enumerate(others):
        k_m.append(rcopy(mown, mall.at[me], ms.at[i], mr.at[i], peer(m), mate if o else core))
        k_m[-1].start()

    k_g.wait_recv()
    for k in k_n:
        k.wait_recv()
    ga[:, :D] = tn(duall[...], xall[...]) * (1.0 / (N_CHIP * N_CORE * TOK))
    ga[:, D:] = jnp.zeros((R * T, DP - D), F32)
    parts = gram_parts([ga[r * T : (r + 1) * T, :] for r in range(R)])
    for k in k_m:
        k.wait_recv()
    mb = jnp.broadcast_to(sum(mall[i] for i in range(N_CHIP * N_CORE)), (T, 128))
    col = [
        jnp.sum(p + jnp.where(lane == T * k + sub, mb, 0.0), axis=1, keepdims=True) + jnp.zeros((T, 128), F32)
        for k, p in enumerate(parts)
    ]
    scale = jnp.sum(col[0], axis=0, keepdims=True) / T
    col = [c / scale for c in col]
    col += [pltpu.roll(col[T - k], k, 0) for k in range(5, T)]

    def eg_step(_, w):
        grad = sum(col[k] * (w if k == 0 else pltpu.roll(w, k, 0)) for k in range(T))
        w = w * jnp.exp(-grad)
        return w / jnp.sum(w, axis=0, keepdims=True)

    w = lax.fori_loop(0, EG_STEPS, eg_step, jnp.full((T, 128), 1.0 / T, F32))
    alpha_out[...] = jnp.sum(jnp.where(lane == sub, w, 0.0), axis=0, keepdims=True)[:, :T]

    wcol = w[:, 0:1]
    dstart = (D // (N_CHIP * N_CORE)) * me
    dtile = dstart // 128
    da0 = pl.multiple_of(dtile * 128, 128)
    comb_a = jnp.concatenate(
        [jnp.sum(ga[r * T : (r + 1) * T, pl.ds(da0, 256)] * wcol, axis=0, keepdims=True) for r in range(R)], axis=0
    )
    ga_out[...] = pltpu.roll(comb_a, 256 - (dstart - da0), 1)[:, : D // (N_CHIP * N_CORE)]
    comb_b = jnp.concatenate(
        [jnp.sum(gbrecv[r * T : (r + 1) * T, :] * wcol, axis=0, keepdims=True) for r in range(R)], axis=0
    )
    gb_out[...] = pltpu.roll(comb_b, OWIN - off_own, 1)[:, :OWN]

    for k in [k_xp, k_g, k_b] + k_z + k_n + k_m + [k_x[m] for m in k_x] + [k_e[m] for m in k_e] + [k_d[m] for m in k_d]:
        k.wait_send()


def put_kernel(alpha_in, ga_in, gb_in, alpha_out, ga_out, gb_out, sem):
    pairs = ((alpha_in, alpha_out), (ga_in, ga_out), (gb_in, gb_out))
    copies = [pltpu.make_async_copy(a, b, sem.at[i]) for i, (a, b) in enumerate(pairs)]
    for c in copies:
        c.start()
    for c in copies:
        c.wait()


def solution(mesh):
    n_dev = mesh.shape["data"]
    assert n_dev == N_CHIP * N_CORE
    vm = pltpu.VMEM
    dma = pltpu.SemaphoreType.DMA
    scratch = [
        vm((D, HALF), BF16), vm((D, HALF), BF16), vm((D, WIN + R * T), BF16), vm((D, WIN), BF16),
        vm((R, HALF), BF16), vm((R, WIN), BF16), vm((R, D), BF16), vm((T, C, D), BF16), vm((T, TOK), jnp.int32),
        vm((2 * TOK, D), BF16), vm((n_dev * TOK, D), BF16), vm((2 * TOK, HALF), BF16),
        vm((C * T, D), F32), vm((C * T, D), BF16), vm((C * T, D), BF16),
        vm((WIN, R * T), BF16), vm((R * T, WIN), BF16),
        vm((N_CHIP * TOK, R * T), BF16), vm((N_CHIP * TOK, WIN), F32),
        vm((TOK, D), F32), vm((TOK, D), F32), vm((TOK, D), F32),
        vm((TOK, 128), BF16), vm((N_CHIP * TOK, 128), BF16),
        vm((4, T * TOK, D), BF16), vm((N_CHIP * T * TOK, WIN), BF16), vm((N_CHIP * T * TOK, R * T), BF16),
        vm((N_CHIP, TOK, R * T), F32), vm((N_CHIP, TOK, R * T), F32),
        vm((TOK, R * T), BF16), vm((n_dev * TOK, R * T), BF16),
        vm((R * T, WIN), F32), vm((R * T, OWIN), F32),
        vm((1, 128), F32), vm((n_dev, 1, 128), F32), vm((R * T, DP), F32),
        dma((16,)), dma((N_CHIP,)), dma((N_CHIP,)), dma, dma, dma((4,)), dma((4,)),
        dma((N_CHIP,)), dma((N_CHIP,)), dma((N_CHIP,)), dma((N_CHIP,)), dma, dma,
        dma((n_dev,)), dma((n_dev,)), dma((n_dev,)), dma((n_dev,)), dma, dma,
    ]

    def device_step(tokens, labels, w_one, w_two, adapter_a, adapter_b, task_heads):
        out_shapes = ((1, T), (R, D // n_dev), (R, FF // n_dev))
        call = pl.pallas_call(
            kernel,
            out_shape=tuple(pltpu.VMEM(s, F32) for s in out_shapes),
            in_specs=[pl.BlockSpec(memory_space=pltpu.HBM)] * 7,
            out_specs=tuple([pl.BlockSpec(memory_space=pltpu.VMEM)] * 3),
            scratch_shapes=scratch,
            compiler_params=pltpu.CompilerParams(
                collective_id=0, has_side_effects=True, vmem_limit_bytes=60 * 1024 * 1024
            ),
            name="min_norm",
        )
        put = pl.pallas_call(
            put_kernel,
            out_shape=tuple(jax.ShapeDtypeStruct(s, F32) for s in out_shapes),
            in_specs=[pl.BlockSpec(memory_space=pltpu.VMEM)] * 3,
            out_specs=tuple([pl.BlockSpec(memory_space=pltpu.HBM)] * 3),
            scratch_shapes=[dma((3,))],
            compiler_params=pltpu.CompilerParams(vmem_limit_bytes=1024 * 1024),
            name="put",
        )
        results = call(
            tokens, labels, w_one, w_two.T, adapter_a.T, adapter_b, task_heads.transpose(0, 2, 1)
        )
        alpha, ga_t, gb = put(*results)
        return alpha.reshape(T), ga_t.T, gb

    return jax.shard_map(
        device_step,
        mesh=mesh,
        in_specs=(P("data", None), P(None, "data"), P(), P(), P(), P(), P()),
        out_specs=(P(), P("data", None), P(None, "data")),
        check_vma=False,
    )
```

```python
import jax
import jax.numpy as jnp
from jax import lax
from jax.experimental import pallas as pl
from jax.experimental.pallas import tpu as pltpu
from jax.sharding import PartitionSpec as P

EG_STEPS = 20
_cur = [None]


def ph(name):
    if _cur[0] is not None:
        _cur[0].__exit__(None, None, None)
    _cur[0] = jax.named_scope(name) if name else None
    if name:
        _cur[0].__enter__()
F32 = jnp.float32
BF16 = jnp.bfloat16
MESH = pl.DeviceIdType.MESH

N_CHIP, N_CORE = 8, 2
TOK = 32
D, FF, R, T, C = 1600, 6400, 16, 8, 2
DP = 1664
HALF = FF // N_CORE
BLK = FF // N_CHIP
OWN = BLK // N_CORE
WIN = 896
OWIN = 512
W1_CHUNKS = ((0, 1536), (1536, 1664))
W2_CHUNKS = ((0, 512), (512, 512), (1024, 576))
NEAR, FAR = (0, 1, 2, 4), (3, 5, 6, 7)
BLOCKS = ((1, 2), (3, 5, 6, 7), (4,), (0,))
GELU_C = 0.7978845608028654
N_TILE = 256


def nt(a, b):
    return lax.dot_general(a, b, (((1,), (1,)), ((), ())), preferred_element_type=F32)


def tn(a, b):
    return lax.dot_general(a, b, (((0,), (0,)), ((), ())), preferred_element_type=F32)


def nn(a, b):
    return jnp.dot(a, b, preferred_element_type=F32)


def gelu(p):
    th = jnp.tanh(GELU_C * (p + 0.044715 * (p * p * p)))
    return p * (0.5 * (1.0 + th))


def gelu_slope(p):
    p2 = p * p
    th = jnp.tanh(GELU_C * (p + 0.044715 * (p2 * p)))
    return 0.5 * (1.0 + th) + (0.5 * p * (1.0 - th * th)) * (GELU_C * (1.0 + 0.134145 * p2))


def iota(shape, dim):
    return lax.broadcasted_iota(jnp.int32, shape, dim)


def gram_parts(blocks):
    acc = [None] * 5
    for v in blocks:
        for k in range(5):
            w = v * (v if k == 0 else pltpu.roll(v, k, 0))
            w = sum(w[:, i : i + 128] for i in range(0, w.shape[1], 128))
            acc[k] = w if acc[k] is None else acc[k] + w
    return acc


def kernel(
    x_hbm, lab_hbm, w1_hbm, w2_hbm, at_hbm, bm_hbm, hd_hbm,
    alpha_out, ga_out, gb_out,
    w1h, w2h, w1w, w2w, bmh, bmw, at, hd, lab, xp, xall, hbuf, hs, ha, hb, bmt, bms, urep, g,
    zown, zsend, zrecv, eown, eall, dz, dp, ub, dsend, drecv, duown, duall, gb, gbrecv, mown, mall, ga,
    lsem, xs, xr, ps, pr, zs, zr, es, er, ds_, dr, bs, br, ns, nr, ms, mr, gs, gr,
):
    me = lax.axis_index("data")
    chip, core = me // N_CORE, me % N_CORE
    cx, cy, cz = chip % 2, (chip // 2) % 2, chip // 4
    mate = 1 - core

    def peer(m):
        px = 1 - cx if m & 1 else cx
        py = 1 - cy if m & 2 else cy
        pz = 1 - cz if m & 4 else cz
        return 4 * pz + 2 * py + px

    def rcopy(src, dst, ssem, rsem, chip_to, core_to):
        return pltpu.make_async_remote_copy(
            src_ref=src, dst_ref=dst, send_sem=ssem, recv_sem=rsem,
            device_id=(N_CORE * chip_to + core_to,), device_id_type=MESH,
        )

    n_sem = [0]

    def load(src, dst):
        c = pltpu.make_async_copy(src, dst, lsem.at[n_sem[0]])
        n_sem[0] += 1
        c.start()
        return c

    ph("prologue")
    half0 = pl.multiple_of(core * HALF, 128)
    tile0 = (BLK * chip) // 128
    win0 = pl.multiple_of(tile0 * 128, 128)
    off = BLK * chip - win0
    c_x = load(x_hbm, xp.at[pl.ds(0, TOK)])
    c_at = load(at_hbm, at)
    c_hd = load(hd_hbm, hd)
    c_lab = load(lab_hbm, lab)
    c_bmh = load(bm_hbm.at[:, pl.ds(half0, HALF)], bmh)
    c_bmw = load(bm_hbm.at[:, pl.ds(win0, WIN)], bmw)
    c_w1 = [load(w1_hbm.at[:, pl.ds(pl.multiple_of(half0 + a, 128), n)], w1h.at[:, pl.ds(a, n)]) for a, n in W1_CHUNKS]
    c_w2 = [load(w2_hbm.at[pl.ds(a, n), pl.ds(half0, HALF)], w2h.at[pl.ds(a, n)]) for a, n in W2_CHUNKS]
    c_w1w = load(w1_hbm.at[:, pl.ds(win0, WIN)], w1w.at[:, pl.ds(0, WIN)])
    c_w2w = load(w2_hbm.at[:, pl.ds(win0, WIN)], w2w)

    ph("barsig")
    barrier = pltpu.get_barrier_semaphore()
    for m in range(N_CHIP):
        for other in range(N_CORE):
            if m or other:
                pl.semaphore_signal(
                    barrier, inc=1, device_id=(N_CORE * peer(m) + (mate if other else core),), device_id_type=MESH
                )

    eown[...] = jnp.zeros_like(eown)
    row_of_r = (iota((R, R * T), 1) // T == iota((R, R * T), 0)).astype(F32).astype(BF16)
    c_hd.wait()
    for t in range(T):
        v = hd[t].astype(F32)
        for c in range(C):
            hs[pl.ds(c * T + t, 1), :] = v[c : c + 1]
    ha[...] = hs[...].astype(BF16)
    hb[...] = jnp.concatenate([hs[T:, :], hs[:T, :]], axis=0).astype(BF16)
    c_lab.wait()
    lab_f = lab[...].astype(F32)
    eye = (iota((TOK, TOK), 0) == iota((TOK, TOK), 1)).astype(F32).astype(BF16)
    lab_t = nt(eye, jnp.concatenate([lab_f, lab_f], axis=0).astype(BF16))
    onehot = (lab_t == (iota((TOK, C * T), 1) // T).astype(F32)).astype(F32)
    c_x.wait()
    my_row = pl.multiple_of(core * (N_CHIP * TOK) + chip * TOK, TOK)
    xall[pl.ds(my_row, TOK), :] = xp[pl.ds(0, TOK), :]

    ph("barwait")
    pl.semaphore_wait(barrier, N_CHIP * N_CORE - 1)

    ph("sends")
    k_xp = rcopy(xp.at[pl.ds(0, TOK)], xp.at[pl.ds(TOK, TOK)], ps, pr, chip, mate)
    k_xp.start()
    k_x = {}
    for m in (1, 2, 4, 7):
        k_x[m] = rcopy(xp.at[pl.ds(0, TOK)], xall.at[pl.ds(my_row, TOK)], xs.at[m], xr.at[m], peer(m), core)
        k_x[m].start()

    ph("prep2")
    c_at.wait()
    w1w[:, WIN:] = tn(at[...], row_of_r).astype(BF16)
    c_bmw.wait()
    colw = iota((R, WIN), 1)
    bm_f = jnp.where((colw >= off) & (colw < off + BLK), bmw[...].astype(F32), 0.0)
    bmt[...] = tn(bm_f.astype(BF16), row_of_r).astype(BF16)
    first_of_r = (T * iota((R, R * T), 0) == iota((R, R * T), 1)).astype(F32).astype(BF16)
    bms[...] = tn(first_of_r, bmw[...]).astype(BF16)

    ph("w_xp")
    k_xp.wait_recv()
    ph("u2")
    x2 = xp[...]
    u2 = nt(x2, at[...]).astype(BF16)
    c_bmh.wait()
    for (a, n), cp in zip(W1_CHUNKS, c_w1):
        ph("w_w1")
        cp.wait()
        ph("p1")
        for i in range(a, a + n, N_TILE):
            j = min(i + N_TILE, a + n)
            pre = nn(x2, w1h[:, i:j]) + nn(u2, bmh[:, i:j])
            hbuf[:, i:j] = gelu(pre).astype(BF16)
    k_z = []
    grp_row = pl.multiple_of(core * (N_CHIP * TOK), N_CHIP * TOK)

    def relay():
        ph("w_xnear")
        for got in (1, 2, 4):
            k_x[got].wait_recv()
        ph("relay")
        for got, to in ((1, 2), (2, 4), (4, 1)):
            rows = xall.at[pl.ds(pl.multiple_of(grp_row + peer(got) * TOK, TOK), TOK)]
            k_x[got + to] = rcopy(rows, rows, xs.at[got + to], xr.at[got + to], peer(to), core)
            k_x[got + to].start()

    for i, ((a, n), cp) in enumerate(zip(W2_CHUNKS, c_w2)):
        ph("w_w2")
        cp.wait()
        ph("p2")
        for j in range(a, a + n, N_TILE):
            z = nt(hbuf[...], w2h[j : min(j + N_TILE, a + n), :])
            zown[:, j : min(j + N_TILE, a + n)] = z[:TOK]
            zsend[:, j : min(j + N_TILE, a + n)] = z[TOK:]
        k_z.append(rcopy(zsend.at[:, pl.ds(a, n)], zrecv.at[:, pl.ds(a, n)], zs.at[i], zr.at[i], chip, mate))
        k_z[-1].start()
        if i == 0:
            relay()

    ph("w_w1w")
    c_w1w.wait()

    def slopes(which, base):
        ph("w_x")
        for m in which:
            if m in FAR:
                k_x[m].wait_recv()
        ph("slp")
        xc = jnp.concatenate(
            [xall[pl.ds(pl.multiple_of(grp_row + peer(m) * TOK, TOK), TOK), :] for m in which], axis=0
        )
        n_row = len(which) * TOK
        last = WIN - WIN % N_TILE
        pre = nn(xc, w1w[:, last:])
        ur = pre[:, WIN - last :].astype(BF16)
        urep[base : base + n_row, :] = ur
        pre = pre[:, : WIN - last] + nn(ur, bms[:, last:])
        g[base : base + n_row, last:] = gelu_slope(pre)
        for a in range(0, last, N_TILE):
            pre = nn(xc, w1w[:, a : a + N_TILE]) + nn(ur, bms[:, a : a + N_TILE])
            g[base : base + n_row, a : a + N_TILE] = gelu_slope(pre)

    slopes(NEAR, 0)
    ph("w_z")
    for k in k_z:
        k.wait_recv()
    ph("logits")
    xf = xp[pl.ds(0, TOK), :].astype(F32)
    zb = (xf + (zown[...] + zrecv[...])).astype(BF16)
    la, lb = nt(zb, ha[...]), nt(zb, hb[...])
    top = jnp.maximum(la, lb)
    ea, eb = jnp.exp(la - top), jnp.exp(lb - top)
    err = (ea / (ea + eb) - onehot).astype(BF16)
    eown[:, : C * T] = err
    my_slot = pl.multiple_of(chip * TOK, TOK)
    eall[pl.ds(my_slot, TOK), :] = eown[...]
    ph("esend")
    k_e = {}
    for m in (1, 2, 4, 3, 5, 6, 7):
        k_e[m] = rcopy(eown, eall.at[pl.ds(my_slot, TOK)], es.at[m], er.at[m], peer(m), core)
        k_e[m].start()

    ph("w_w2w")
    c_w2w.wait()
    lane_t = iota((TOK, R * T), 1) % T
    rel = {m: i * TOK for i, m in enumerate(NEAR + FAR)}
    k_d = {}

    def backward(block):
        ph("w_e")
        for m in block:
            if m:
                k_e[m].wait_recv()
        ph("back")
        dus = {}
        for m in block:
            r0 = rel[m] * T
            e = eall[pl.ds(pl.multiple_of(peer(m) * TOK, TOK), TOK), :].astype(F32)
            for t in range(T):
                dz[rel[m] // TOK % 4, t * TOK : (t + 1) * TOK, :] = (
                    e[:, t : t + 1] * hs[pl.ds(t, 1), :] + e[:, T + t : T + t + 1] * hs[pl.ds(T + t, 1), :]
                ).astype(BF16)
            for a in range(0, WIN, N_TILE):
                n = min(N_TILE, WIN - a)
                dh = nn(dz[rel[m] // TOK % 4], w2w[:, a : a + n]).reshape(T, TOK, n)
                slope = g[rel[m] : rel[m] + TOK, a : a + n]
                dp[r0 : r0 + T * TOK, a : a + n] = (dh * slope[None]).astype(BF16).reshape(T * TOK, n)
            du = nn(dp[r0 : r0 + T * TOK, :], bmt[...])
            dus[m] = sum(jnp.where(lane_t == t, du[t * TOK : (t + 1) * TOK], 0.0) for t in range(T))
            if m:
                dsend[m] = dus[m]
            ur = urep[rel[m] : rel[m] + TOK, :].astype(F32)
            for t in range(T):
                ub[r0 + t * TOK : r0 + (t + 1) * TOK, :] = jnp.where(lane_t == t, ur, 0.0).astype(BF16)
        for m in block:
            if m:
                k_d[m] = rcopy(dsend.at[m], drecv.at[m], ds_.at[m], dr.at[m], peer(m), core)
                k_d[m].start()
        return dus

    slopes(FAR, len(NEAR) * TOK)
    k_g = rcopy(xall.at[pl.ds(grp_row, N_CHIP * TOK)], xall.at[pl.ds(grp_row, N_CHIP * TOK)], gs, gr, chip, mate)
    k_g.start()
    for block in BLOCKS[:-1]:
        backward(block)
    du_own = backward(BLOCKS[-1])[0]
    ph("gb")
    for a in range(0, WIN, N_TILE):
        gb[:, a : min(a + N_TILE, WIN)] = tn(ub[...], dp[:, a : min(a + N_TILE, WIN)])

    ph("gbsend")
    ow0 = pl.multiple_of(core * (OWIN - 128), 128)
    mw0 = pl.multiple_of(mate * (OWIN - 128), 128)
    k_b = rcopy(gb.at[:, pl.ds(mw0, OWIN)], gbrecv, bs, br, chip, mate)
    k_b.start()
    ph("w_du")
    for m in range(1, N_CHIP):
        k_d[m].wait_recv()
        du_own = du_own + drecv[m]
    ph("duag")
    duown[...] = du_own.astype(BF16)
    duall[pl.ds(my_row, TOK), :] = duown[...]
    others = [(m, o) for m in (7, 6, 5, 3, 4, 2, 1, 0) for o in range(N_CORE) if m or o]
    k_n = []
    for i, (m, o) in enumerate(others):
        k_n.append(rcopy(duown, duall.at[pl.ds(my_row, TOK)], ns.at[i], nr.at[i], peer(m), mate if o else core))
        k_n[-1].start()

    ph("w_gb")
    k_b.wait_recv()
    ph("gramb")
    off_own = off + 16 * core
    colo = iota((R * T, OWIN), 1)
    shard = (gb[:, pl.ds(ow0, OWIN)] + gbrecv[...]) * (1.0 / (N_CHIP * N_CORE * TOK))
    shard = jnp.where((colo >= off_own) & (colo < off_own + OWN), shard, 0.0)
    gbrecv[...] = shard
    lane = iota((T, 128), 1)
    sub = iota((T, 128), 0)
    parts = gram_parts([gbrecv[r * T : (r + 1) * T, :] for r in range(R)])
    row = sum(
        jnp.where(lane == T * k + sub, jnp.sum(p, axis=1, keepdims=True), 0.0) for k, p in enumerate(parts)
    )
    mown[...] = jnp.sum(row, axis=0, keepdims=True)
    mall[me] = mown[...]
    k_m = []
    for i, (m, o) in enumerate(others):
        k_m.append(rcopy(mown, mall.at[me], ms.at[i], mr.at[i], peer(m), mate if o else core))
        k_m[-1].start()

    ph("w_g")
    k_g.wait_recv()
    ph("w_duag")
    for k in k_n:
        k.wait_recv()
    ph("ga")
    ga[:, :D] = tn(duall[...], xall[...]) * (1.0 / (N_CHIP * N_CORE * TOK))
    ga[:, D:] = jnp.zeros((R * T, DP - D), F32)
    parts = gram_parts([ga[r * T : (r + 1) * T, :] for r in range(R)])
    ph("w_m")
    for k in k_m:
        k.wait_recv()
    ph("msum")
    mb = jnp.broadcast_to(sum(mall[i] for i in range(N_CHIP * N_CORE)), (T, 128))
    col = [
        jnp.sum(p + jnp.where(lane == T * k + sub, mb, 0.0), axis=1, keepdims=True) + jnp.zeros((T, 128), F32)
        for k, p in enumerate(parts)
    ]
    scale = jnp.sum(col[0], axis=0, keepdims=True) / T
    col = [c / scale for c in col]
    col += [pltpu.roll(col[T - k], k, 0) for k in range(5, T)]

    def eg_step(_, w):
        grad = sum(col[k] * (w if k == 0 else pltpu.roll(w, k, 0)) for k in range(T))
        w = w * jnp.exp(-grad)
        return w / jnp.sum(w, axis=0, keepdims=True)

    ph("eg")
    w = lax.fori_loop(0, EG_STEPS, eg_step, jnp.full((T, 128), 1.0 / T, F32))
    ph("out")
    alpha_out[...] = jnp.sum(jnp.where(lane == sub, w, 0.0), axis=0, keepdims=True)[:, :T]

    wcol = w[:, 0:1]
    dstart = (D // (N_CHIP * N_CORE)) * me
    dtile = dstart // 128
    da0 = pl.multiple_of(dtile * 128, 128)
    comb_a = jnp.concatenate(
        [jnp.sum(ga[r * T : (r + 1) * T, pl.ds(da0, 256)] * wcol, axis=0, keepdims=True) for r in range(R)], axis=0
    )
    ga_out[...] = pltpu.roll(comb_a, 256 - (dstart - da0), 1)[:, : D // (N_CHIP * N_CORE)]
    comb_b = jnp.concatenate(
        [jnp.sum(gbrecv[r * T : (r + 1) * T, :] * wcol, axis=0, keepdims=True) for r in range(R)], axis=0
    )
    gb_out[...] = pltpu.roll(comb_b, OWIN - off_own, 1)[:, :OWN]

    ph("w_send")
    for k in [k_xp, k_g, k_b] + k_z + k_n + k_m + [k_x[m] for m in k_x] + [k_e[m] for m in k_e] + [k_d[m] for m in k_d]:
        k.wait_send()
    ph(None)


def put_kernel(alpha_in, ga_in, gb_in, alpha_out, ga_out, gb_out, sem):
    pairs = ((alpha_in, alpha_out), (ga_in, ga_out), (gb_in, gb_out))
    copies = [pltpu.make_async_copy(a, b, sem.at[i]) for i, (a, b) in enumerate(pairs)]
    for c in copies:
        c.start()
    for c in copies:
        c.wait()


def solution(mesh):
    n_dev = mesh.shape["data"]
    assert n_dev == N_CHIP * N_CORE
    vm = pltpu.VMEM
    dma = pltpu.SemaphoreType.DMA
    scratch = [
        vm((D, HALF), BF16), vm((D, HALF), BF16), vm((D, WIN + R * T), BF16), vm((D, WIN), BF16),
        vm((R, HALF), BF16), vm((R, WIN), BF16), vm((R, D), BF16), vm((T, C, D), BF16), vm((T, TOK), jnp.int32),
        vm((2 * TOK, D), BF16), vm((n_dev * TOK, D), BF16), vm((2 * TOK, HALF), BF16),
        vm((C * T, D), F32), vm((C * T, D), BF16), vm((C * T, D), BF16),
        vm((WIN, R * T), BF16), vm((R * T, WIN), BF16),
        vm((N_CHIP * TOK, R * T), BF16), vm((N_CHIP * TOK, WIN), F32),
        vm((TOK, D), F32), vm((TOK, D), F32), vm((TOK, D), F32),
        vm((TOK, 128), BF16), vm((N_CHIP * TOK, 128), BF16),
        vm((4, T * TOK, D), BF16), vm((N_CHIP * T * TOK, WIN), BF16), vm((N_CHIP * T * TOK, R * T), BF16),
        vm((N_CHIP, TOK, R * T), F32), vm((N_CHIP, TOK, R * T), F32),
        vm((TOK, R * T), BF16), vm((n_dev * TOK, R * T), BF16),
        vm((R * T, WIN), F32), vm((R * T, OWIN), F32),
        vm((1, 128), F32), vm((n_dev, 1, 128), F32), vm((R * T, DP), F32),
        dma((16,)), dma((N_CHIP,)), dma((N_CHIP,)), dma, dma, dma((4,)), dma((4,)),
        dma((N_CHIP,)), dma((N_CHIP,)), dma((N_CHIP,)), dma((N_CHIP,)), dma, dma,
        dma((n_dev,)), dma((n_dev,)), dma((n_dev,)), dma((n_dev,)), dma, dma,
    ]

    def device_step(tokens, labels, w_one, w_two, adapter_a, adapter_b, task_heads):
        out_shapes = ((1, T), (R, D // n_dev), (R, FF // n_dev))
        call = pl.pallas_call(
            kernel,
            out_shape=tuple(pltpu.VMEM(s, F32) for s in out_shapes),
            in_specs=[pl.BlockSpec(memory_space=pltpu.HBM)] * 7,
            out_specs=tuple([pl.BlockSpec(memory_space=pltpu.VMEM)] * 3),
            scratch_shapes=scratch,
            compiler_params=pltpu.CompilerParams(
                collective_id=0, has_side_effects=True, vmem_limit_bytes=60 * 1024 * 1024
            ),
            name="min_norm",
        )
        put = pl.pallas_call(
            put_kernel,
            out_shape=tuple(jax.ShapeDtypeStruct(s, F32) for s in out_shapes),
            in_specs=[pl.BlockSpec(memory_space=pltpu.VMEM)] * 3,
            out_specs=tuple([pl.BlockSpec(memory_space=pltpu.HBM)] * 3),
            scratch_shapes=[dma((3,))],
            compiler_params=pltpu.CompilerParams(vmem_limit_bytes=1024 * 1024),
            name="put",
        )
        results = call(
            tokens, labels, w_one, w_two.T, adapter_a.T, adapter_b, task_heads.transpose(0, 2, 1)
        )
        alpha, ga_t, gb = put(*results)
        return alpha.reshape(T), ga_t.T, gb

    return jax.shard_map(
        device_step,
        mesh=mesh,
        in_specs=(P("data", None), P(None, "data"), P(), P(), P(), P(), P()),
        out_specs=(P(), P("data", None), P(None, "data")),
        check_vma=False,
    )
```

```python
import jax
import jax.numpy as jnp
from jax import lax
from jax.experimental import pallas as pl
from jax.experimental.pallas import tpu as pltpu
from jax.sharding import PartitionSpec as P

EG_STEPS = 20
F32 = jnp.float32
BF16 = jnp.bfloat16
MESH = pl.DeviceIdType.MESH

N_CHIP, N_CORE = 8, 2
TOK = 32
D, FF, R, T, C = 1600, 6400, 16, 8, 2
DP = 1664
HALF = FF // N_CORE
BLK = FF // N_CHIP
OWN = BLK // N_CORE
WIN = 896
OWIN = 512
W1_CHUNKS = ((0, 1536), (1536, 1664))
W2_CHUNKS = ((0, 512), (512, 512), (1024, 576))
NEAR, FAR = (0, 1, 2, 4), (3, 5, 6, 7)
BLOCKS = ((1, 2), (3, 5, 6, 7), (4,), (0,))
GELU_C = 0.7978845608028654
N_TILE = 256


def nt(a, b):
    return lax.dot_general(a, b, (((1,), (1,)), ((), ())), preferred_element_type=F32)


def tn(a, b):
    return lax.dot_general(a, b, (((0,), (0,)), ((), ())), preferred_element_type=F32)


def nn(a, b):
    return jnp.dot(a, b, preferred_element_type=F32)


def gelu(p):
    th = jnp.tanh(GELU_C * (p + 0.044715 * (p * p * p)))
    return p * (0.5 * (1.0 + th))


def gelu_slope(p):
    p2 = p * p
    th = jnp.tanh(GELU_C * (p + 0.044715 * (p2 * p)))
    return 0.5 * (1.0 + th) + (0.5 * p * (1.0 - th * th)) * (GELU_C * (1.0 + 0.134145 * p2))


def iota(shape, dim):
    return lax.broadcasted_iota(jnp.int32, shape, dim)


def gram_parts(blocks):
    acc = [None] * 5
    for v in blocks:
        for k in range(5):
            w = v * (v if k == 0 else pltpu.roll(v, k, 0))
            w = sum(w[:, i : i + 128] for i in range(0, w.shape[1], 128))
            acc[k] = w if acc[k] is None else acc[k] + w
    return acc


def kernel(
    x_hbm, lab_hbm, w1_hbm, w2_hbm, at_hbm, bm_hbm, hd_hbm,
    alpha_out, ga_out, gb_out,
    w1h, w2h, w1w, w2w, bmh, bmw, at, hd, lab, xp, xall, hbuf, hs, ha, hb, bmt, bms, urep, g,
    zown, zsend, zrecv, eown, eall, dz, dp, ub, dsend, drecv, duown, duall, gb, gbrecv, mown, mall, ga,
    lsem, xs, xr, ps, pr, zs, zr, es, er, ds_, dr, bs, br, ns, nr, ms, mr, gs, gr,
):
    me = lax.axis_index("data")
    chip, core = me // N_CORE, me % N_CORE
    cx, cy, cz = chip % 2, (chip // 2) % 2, chip // 4
    mate = 1 - core

    def peer(m):
        px = 1 - cx if m & 1 else cx
        py = 1 - cy if m & 2 else cy
        pz = 1 - cz if m & 4 else cz
        return 4 * pz + 2 * py + px

    def rcopy(src, dst, ssem, rsem, chip_to, core_to):
        return pltpu.make_async_remote_copy(
            src_ref=src, dst_ref=dst, send_sem=ssem, recv_sem=rsem,
            device_id=(N_CORE * chip_to + core_to,), device_id_type=MESH,
        )

    n_sem = [0]

    def load(src, dst):
        c = pltpu.make_async_copy(src, dst, lsem.at[n_sem[0]])
        n_sem[0] += 1
        c.start()
        return c

    half0 = pl.multiple_of(core * HALF, 128)
    tile0 = (BLK * chip) // 128
    win0 = pl.multiple_of(tile0 * 128, 128)
    off = BLK * chip - win0
    c_x = load(x_hbm, xp.at[pl.ds(0, TOK)])
    c_at = load(at_hbm, at)
    c_hd = load(hd_hbm, hd)
    c_lab = load(lab_hbm, lab)
    c_bmh = load(bm_hbm.at[:, pl.ds(half0, HALF)], bmh)
    c_bmw = load(bm_hbm.at[:, pl.ds(win0, WIN)], bmw)
    c_w1 = [load(w1_hbm.at[:, pl.ds(pl.multiple_of(half0 + a, 128), n)], w1h.at[:, pl.ds(a, n)]) for a, n in W1_CHUNKS]
    c_w2 = [load(w2_hbm.at[pl.ds(a, n), pl.ds(half0, HALF)], w2h.at[pl.ds(a, n)]) for a, n in W2_CHUNKS]
    c_w1w = load(w1_hbm.at[:, pl.ds(win0, WIN)], w1w.at[:, pl.ds(0, WIN)])
    c_w2w = load(w2_hbm.at[:, pl.ds(win0, WIN)], w2w)

    barrier = pltpu.get_barrier_semaphore()
    for m in range(N_CHIP):
        for other in range(N_CORE):
            if m or other:
                pl.semaphore_signal(
                    barrier, inc=1, device_id=(N_CORE * peer(m) + (mate if other else core),), device_id_type=MESH
                )

    eown[...] = jnp.zeros_like(eown)
    row_of_r = (iota((R, R * T), 1) // T == iota((R, R * T), 0)).astype(F32).astype(BF16)
    c_hd.wait()
    for t in range(T):
        v = hd[t].astype(F32)
        for c in range(C):
            hs[pl.ds(c * T + t, 1), :] = v[c : c + 1]
    ha[...] = hs[...].astype(BF16)
    hb[...] = jnp.concatenate([hs[T:, :], hs[:T, :]], axis=0).astype(BF16)
    c_lab.wait()
    lab_f = lab[...].astype(F32)
    eye = (iota((TOK, TOK), 0) == iota((TOK, TOK), 1)).astype(F32).astype(BF16)
    lab_t = nt(eye, jnp.concatenate([lab_f, lab_f], axis=0).astype(BF16))
    onehot = (lab_t == (iota((TOK, C * T), 1) // T).astype(F32)).astype(F32)
    c_x.wait()
    my_row = pl.multiple_of(core * (N_CHIP * TOK) + chip * TOK, TOK)
    xall[pl.ds(my_row, TOK), :] = xp[pl.ds(0, TOK), :]

    pl.semaphore_wait(barrier, N_CHIP * N_CORE - 1)

    k_xp = rcopy(xp.at[pl.ds(0, TOK)], xp.at[pl.ds(TOK, TOK)], ps, pr, chip, mate)
    k_xp.start()
    k_x = {}
    for m in (1, 2, 4, 7):
        k_x[m] = rcopy(xp.at[pl.ds(0, TOK)], xall.at[pl.ds(my_row, TOK)], xs.at[m], xr.at[m], peer(m), core)
        if m != 7:
            k_x[m].start()

    c_at.wait()
    w1w[:, WIN:] = tn(at[...], row_of_r).astype(BF16)
    c_bmw.wait()
    colw = iota((R, WIN), 1)
    bm_f = jnp.where((colw >= off) & (colw < off + BLK), bmw[...].astype(F32), 0.0)
    bmt[...] = tn(bm_f.astype(BF16), row_of_r).astype(BF16)
    first_of_r = (T * iota((R, R * T), 0) == iota((R, R * T), 1)).astype(F32).astype(BF16)
    bms[...] = tn(first_of_r, bmw[...]).astype(BF16)

    k_xp.wait_recv()
    x2 = xp[...]
    u2 = nt(x2, at[...]).astype(BF16)
    c_bmh.wait()
    for (a, n), cp in zip(W1_CHUNKS, c_w1):
        cp.wait()
        for i in range(a, a + n, N_TILE):
            j = min(i + N_TILE, a + n)
            pre = nn(x2, w1h[:, i:j]) + nn(u2, bmh[:, i:j])
            hbuf[:, i:j] = gelu(pre).astype(BF16)
        if a == 0:
            k_x[7].start()
    k_z = []
    grp_row = pl.multiple_of(core * (N_CHIP * TOK), N_CHIP * TOK)

    def relay():
        for got in (1, 2, 4):
            k_x[got].wait_recv()
        for got, to in ((1, 2), (2, 4), (4, 1)):
            rows = xall.at[pl.ds(pl.multiple_of(grp_row + peer(got) * TOK, TOK), TOK)]
            k_x[got + to] = rcopy(rows, rows, xs.at[got + to], xr.at[got + to], peer(to), core)
            k_x[got + to].start()

    for i, ((a, n), cp) in enumerate(zip(W2_CHUNKS, c_w2)):
        cp.wait()
        for j in range(a, a + n, N_TILE):
            z = nt(hbuf[...], w2h[j : min(j + N_TILE, a + n), :])
            zown[:, j : min(j + N_TILE, a + n)] = z[:TOK]
            zsend[:, j : min(j + N_TILE, a + n)] = z[TOK:]
        k_z.append(rcopy(zsend.at[:, pl.ds(a, n)], zrecv.at[:, pl.ds(a, n)], zs.at[i], zr.at[i], chip, mate))
        k_z[-1].start()
        if i == 0:
            relay()

    c_w1w.wait()

    def slopes(which, base):
        for m in which:
            if m in FAR:
                k_x[m].wait_recv()
        xc = jnp.concatenate(
            [xall[pl.ds(pl.multiple_of(grp_row + peer(m) * TOK, TOK), TOK), :] for m in which], axis=0
        )
        n_row = len(which) * TOK
        last = WIN - WIN % N_TILE
        pre = nn(xc, w1w[:, last:])
        ur = pre[:, WIN - last :].astype(BF16)
        urep[base : base + n_row, :] = ur
        pre = pre[:, : WIN - last] + nn(ur, bms[:, last:])
        g[base : base + n_row, last:] = gelu_slope(pre)
        for a in range(0, last, N_TILE):
            pre = nn(xc, w1w[:, a : a + N_TILE]) + nn(ur, bms[:, a : a + N_TILE])
            g[base : base + n_row, a : a + N_TILE] = gelu_slope(pre)

    slopes(NEAR, 0)
    for k in k_z:
        k.wait_recv()
    xf = xp[pl.ds(0, TOK), :].astype(F32)
    zb = (xf + (zown[...] + zrecv[...])).astype(BF16)
    la, lb = nt(zb, ha[...]), nt(zb, hb[...])
    top = jnp.maximum(la, lb)
    ea, eb = jnp.exp(la - top), jnp.exp(lb - top)
    err = (ea / (ea + eb) - onehot).astype(BF16)
    eown[:, : C * T] = err
    my_slot = pl.multiple_of(chip * TOK, TOK)
    eall[pl.ds(my_slot, TOK), :] = eown[...]
    k_e = {}
    for m in (1, 2, 4, 3, 5, 6, 7):
        k_e[m] = rcopy(eown, eall.at[pl.ds(my_slot, TOK)], es.at[m], er.at[m], peer(m), core)
        k_e[m].start()

    c_w2w.wait()
    lane_t = iota((TOK, R * T), 1) % T
    rel = {m: i * TOK for i, m in enumerate(NEAR + FAR)}
    k_d = {}

    def backward(block):
        for m in block:
            if m:
                k_e[m].wait_recv()
        dus = {}
        for m in block:
            r0 = rel[m] * T
            e = eall[pl.ds(pl.multiple_of(peer(m) * TOK, TOK), TOK), :].astype(F32)
            for t in range(T):
                dz[rel[m] // TOK % 4, t * TOK : (t + 1) * TOK, :] = (
                    e[:, t : t + 1] * hs[pl.ds(t, 1), :] + e[:, T + t : T + t + 1] * hs[pl.ds(T + t, 1), :]
                ).astype(BF16)
            for a in range(0, WIN, N_TILE):
                n = min(N_TILE, WIN - a)
                dh = nn(dz[rel[m] // TOK % 4], w2w[:, a : a + n]).reshape(T, TOK, n)
                slope = g[rel[m] : rel[m] + TOK, a : a + n]
                dp[r0 : r0 + T * TOK, a : a + n] = (dh * slope[None]).astype(BF16).reshape(T * TOK, n)
            du = nn(dp[r0 : r0 + T * TOK, :], bmt[...])
            dus[m] = sum(jnp.where(lane_t == t, du[t * TOK : (t + 1) * TOK], 0.0) for t in range(T))
            if m:
                dsend[m] = dus[m]
            ur = urep[rel[m] : rel[m] + TOK, :].astype(F32)
            for t in range(T):
                ub[r0 + t * TOK : r0 + (t + 1) * TOK, :] = jnp.where(lane_t == t, ur, 0.0).astype(BF16)
        for m in block:
            if m:
                k_d[m] = rcopy(dsend.at[m], drecv.at[m], ds_.at[m], dr.at[m], peer(m), core)
                k_d[m].start()
        return dus

    slopes(FAR, len(NEAR) * TOK)
    k_g = rcopy(xall.at[pl.ds(grp_row, N_CHIP * TOK)], xall.at[pl.ds(grp_row, N_CHIP * TOK)], gs, gr, chip, mate)
    k_g.start()
    for block in BLOCKS[:-1]:
        backward(block)
    du_own = backward(BLOCKS[-1])[0]
    for a in range(0, WIN, N_TILE):
        gb[:, a : min(a + N_TILE, WIN)] = tn(ub[...], dp[:, a : min(a + N_TILE, WIN)])

    ow0 = pl.multiple_of(core * (OWIN - 128), 128)
    mw0 = pl.multiple_of(mate * (OWIN - 128), 128)
    k_b = rcopy(gb.at[:, pl.ds(mw0, OWIN)], gbrecv, bs, br, chip, mate)
    k_b.start()
    for m in range(1, N_CHIP):
        k_d[m].wait_recv()
        du_own = du_own + drecv[m]
    duown[...] = du_own.astype(BF16)
    duall[pl.ds(my_row, TOK), :] = duown[...]
    others = [(m, o) for m in (7, 6, 5, 3, 4, 2, 1, 0) for o in range(N_CORE) if m or o]
    k_n = []
    for i, (m, o) in enumerate(others):
        k_n.append(rcopy(duown, duall.at[pl.ds(my_row, TOK)], ns.at[i], nr.at[i], peer(m), mate if o else core))
        k_n[-1].start()

    k_b.wait_recv()
    off_own = off + 16 * core
    colo = iota((R * T, OWIN), 1)
    shard = (gb[:, pl.ds(ow0, OWIN)] + gbrecv[...]) * (1.0 / (N_CHIP * N_CORE * TOK))
    shard = jnp.where((colo >= off_own) & (colo < off_own + OWN), shard, 0.0)
    gbrecv[...] = shard
    lane = iota((T, 128), 1)
    sub = iota((T, 128), 0)
    parts = gram_parts([gbrecv[r * T : (r + 1) * T, :] for r in range(R)])
    row = sum(
        jnp.where(lane == T * k + sub, jnp.sum(p, axis=1, keepdims=True), 0.0) for k, p in enumerate(parts)
    )
    mown[...] = jnp.sum(row, axis=0, keepdims=True)
    mall[me] = mown[...]
    k_m = []
    for i, (m, o) in enumerate(others):
        k_m.append(rcopy(mown, mall.at[me], ms.at[i], mr.at[i], peer(m), mate if o else core))
        k_m[-1].start()

    k_g.wait_recv()
    for k in k_n:
        k.wait_recv()
    ga[:, :D] = tn(duall[...], xall[...]) * (1.0 / (N_CHIP * N_CORE * TOK))
    ga[:, D:] = jnp.zeros((R * T, DP - D), F32)
    parts = gram_parts([ga[r * T : (r + 1) * T, :] for r in range(R)])
    for k in k_m:
        k.wait_recv()
    mb = jnp.broadcast_to(sum(mall[i] for i in range(N_CHIP * N_CORE)), (T, 128))
    col = [
        jnp.sum(p + jnp.where(lane == T * k + sub, mb, 0.0), axis=1, keepdims=True) + jnp.zeros((T, 128), F32)
        for k, p in enumerate(parts)
    ]
    scale = jnp.sum(col[0], axis=0, keepdims=True) / T
    col = [c / scale for c in col]
    col += [pltpu.roll(col[T - k], k, 0) for k in range(5, T)]

    def eg_step(_, w):
        grad = sum(col[k] * (w if k == 0 else pltpu.roll(w, k, 0)) for k in range(T))
        w = w * jnp.exp(-grad)
        return w / jnp.sum(w, axis=0, keepdims=True)

    w = lax.fori_loop(0, EG_STEPS, eg_step, jnp.full((T, 128), 1.0 / T, F32))
    alpha_out[...] = jnp.sum(jnp.where(lane == sub, w, 0.0), axis=0, keepdims=True)[:, :T]

    wcol = w[:, 0:1]
    dstart = (D // (N_CHIP * N_CORE)) * me
    dtile = dstart // 128
    da0 = pl.multiple_of(dtile * 128, 128)
    comb_a = jnp.concatenate(
        [jnp.sum(ga[r * T : (r + 1) * T, pl.ds(da0, 256)] * wcol, axis=0, keepdims=True) for r in range(R)], axis=0
    )
    ga_out[...] = pltpu.roll(comb_a, 256 - (dstart - da0), 1)[:, : D // (N_CHIP * N_CORE)]
    comb_b = jnp.concatenate(
        [jnp.sum(gbrecv[r * T : (r + 1) * T, :] * wcol, axis=0, keepdims=True) for r in range(R)], axis=0
    )
    gb_out[...] = pltpu.roll(comb_b, OWIN - off_own, 1)[:, :OWN]

    for k in [k_xp, k_g, k_b] + k_z + k_n + k_m + [k_x[m] for m in k_x] + [k_e[m] for m in k_e] + [k_d[m] for m in k_d]:
        k.wait_send()


def put_kernel(alpha_in, ga_in, gb_in, alpha_out, ga_out, gb_out, sem):
    pairs = ((alpha_in, alpha_out), (ga_in, ga_out), (gb_in, gb_out))
    copies = [pltpu.make_async_copy(a, b, sem.at[i]) for i, (a, b) in enumerate(pairs)]
    for c in copies:
        c.start()
    for c in copies:
        c.wait()


def solution(mesh):
    n_dev = mesh.shape["data"]
    assert n_dev == N_CHIP * N_CORE
    vm = pltpu.VMEM
    dma = pltpu.SemaphoreType.DMA
    scratch = [
        vm((D, HALF), BF16), vm((D, HALF), BF16), vm((D, WIN + R * T), BF16), vm((D, WIN), BF16),
        vm((R, HALF), BF16), vm((R, WIN), BF16), vm((R, D), BF16), vm((T, C, D), BF16), vm((T, TOK), jnp.int32),
        vm((2 * TOK, D), BF16), vm((n_dev * TOK, D), BF16), vm((2 * TOK, HALF), BF16),
        vm((C * T, D), F32), vm((C * T, D), BF16), vm((C * T, D), BF16),
        vm((WIN, R * T), BF16), vm((R * T, WIN), BF16),
        vm((N_CHIP * TOK, R * T), BF16), vm((N_CHIP * TOK, WIN), F32),
        vm((TOK, D), F32), vm((TOK, D), F32), vm((TOK, D), F32),
        vm((TOK, 128), BF16), vm((N_CHIP * TOK, 128), BF16),
        vm((4, T * TOK, D), BF16), vm((N_CHIP * T * TOK, WIN), BF16), vm((N_CHIP * T * TOK, R * T), BF16),
        vm((N_CHIP, TOK, R * T), F32), vm((N_CHIP, TOK, R * T), F32),
        vm((TOK, R * T), BF16), vm((n_dev * TOK, R * T), BF16),
        vm((R * T, WIN), F32), vm((R * T, OWIN), F32),
        vm((1, 128), F32), vm((n_dev, 1, 128), F32), vm((R * T, DP), F32),
        dma((16,)), dma((N_CHIP,)), dma((N_CHIP,)), dma, dma, dma((4,)), dma((4,)),
        dma((N_CHIP,)), dma((N_CHIP,)), dma((N_CHIP,)), dma((N_CHIP,)), dma, dma,
        dma((n_dev,)), dma((n_dev,)), dma((n_dev,)), dma((n_dev,)), dma, dma,
    ]

    def device_step(tokens, labels, w_one, w_two, adapter_a, adapter_b, task_heads):
        out_shapes = ((1, T), (R, D // n_dev), (R, FF // n_dev))
        call = pl.pallas_call(
            kernel,
            out_shape=tuple(pltpu.VMEM(s, F32) for s in out_shapes),
            in_specs=[pl.BlockSpec(memory_space=pltpu.HBM)] * 7,
            out_specs=tuple([pl.BlockSpec(memory_space=pltpu.VMEM)] * 3),
            scratch_shapes=scratch,
            compiler_params=pltpu.CompilerParams(
                collective_id=0, has_side_effects=True, vmem_limit_bytes=60 * 1024 * 1024
            ),
            name="min_norm",
        )
        put = pl.pallas_call(
            put_kernel,
            out_shape=tuple(jax.ShapeDtypeStruct(s, F32) for s in out_shapes),
            in_specs=[pl.BlockSpec(memory_space=pltpu.VMEM)] * 3,
            out_specs=tuple([pl.BlockSpec(memory_space=pltpu.HBM)] * 3),
            scratch_shapes=[dma((3,))],
            compiler_params=pltpu.CompilerParams(vmem_limit_bytes=1024 * 1024),
            name="put",
        )
        results = call(
            tokens, labels, w_one, w_two.T, adapter_a.T, adapter_b, task_heads.transpose(0, 2, 1)
        )
        alpha, ga_t, gb = put(*results)
        return alpha.reshape(T), ga_t.T, gb

    return jax.shard_map(
        device_step,
        mesh=mesh,
        in_specs=(P("data", None), P(None, "data"), P(), P(), P(), P(), P()),
        out_specs=(P(), P("data", None), P(None, "data")),
        check_vma=False,
    )
```

```python
import jax
import jax.numpy as jnp
from jax import lax
from jax.experimental import pallas as pl
from jax.experimental.pallas import tpu as pltpu
from jax.sharding import PartitionSpec as P

EG_STEPS = 20
F32 = jnp.float32
BF16 = jnp.bfloat16
MESH = pl.DeviceIdType.MESH

N_CHIP, N_CORE = 8, 2
TOK = 32
D, FF, R, T, C = 1600, 6400, 16, 8, 2
DP = 1664
HALF = FF // N_CORE
BLK = FF // N_CHIP
OWN = BLK // N_CORE
WIN = 896
OWIN = 512
W1_CHUNKS = ((0, 1024), (1024, 1024), (2048, 1152))
W2_CHUNKS = ((0, 512), (512, 512), (1024, 576))
NEAR, FAR = (0, 1, 2, 4), (3, 5, 6, 7)
BLOCKS = ((1, 2), (3, 5, 6, 7), (4,), (0,))
GELU_C = 0.7978845608028654
N_TILE = 256


def nt(a, b):
    return lax.dot_general(a, b, (((1,), (1,)), ((), ())), preferred_element_type=F32)


def tn(a, b):
    return lax.dot_general(a, b, (((0,), (0,)), ((), ())), preferred_element_type=F32)


def nn(a, b):
    return jnp.dot(a, b, preferred_element_type=F32)


def gelu(p):
    th = jnp.tanh(GELU_C * (p + 0.044715 * (p * p * p)))
    return p * (0.5 * (1.0 + th))


def gelu_slope(p):
    p2 = p * p
    th = jnp.tanh(GELU_C * (p + 0.044715 * (p2 * p)))
    return 0.5 * (1.0 + th) + (0.5 * p * (1.0 - th * th)) * (GELU_C * (1.0 + 0.134145 * p2))


def iota(shape, dim):
    return lax.broadcasted_iota(jnp.int32, shape, dim)


def gram_parts(blocks):
    acc = [None] * 5
    for v in blocks:
        for k in range(5):
            w = v * (v if k == 0 else pltpu.roll(v, k, 0))
            w = sum(w[:, i : i + 128] for i in range(0, w.shape[1], 128))
            acc[k] = w if acc[k] is None else acc[k] + w
    return acc


def kernel(
    x_hbm, lab_hbm, w1_hbm, w2_hbm, at_hbm, bm_hbm, hd_hbm,
    alpha_out, ga_out, gb_out,
    w1h, w2h, w1w, w2w, bmh, bmw, at, hd, lab, xp, xall, hbuf, hs, ha, hb, bmt, bms, urep, g,
    zown, zsend, zrecv, eown, eall, dz, dp, ub, dsend, drecv, duown, duall, gb, gbrecv, mown, mall, ga,
    lsem, xs, xr, ps, pr, zs, zr, es, er, ds_, dr, bs, br, ns, nr, ms, mr, gs, gr,
):
    me = lax.axis_index("data")
    chip, core = me // N_CORE, me % N_CORE
    cx, cy, cz = chip % 2, (chip // 2) % 2, chip // 4
    mate = 1 - core

    def peer(m):
        px = 1 - cx if m & 1 else cx
        py = 1 - cy if m & 2 else cy
        pz = 1 - cz if m & 4 else cz
        return 4 * pz + 2 * py + px

    def rcopy(src, dst, ssem, rsem, chip_to, core_to):
        return pltpu.make_async_remote_copy(
            src_ref=src, dst_ref=dst, send_sem=ssem, recv_sem=rsem,
            device_id=(N_CORE * chip_to + core_to,), device_id_type=MESH,
        )

    n_sem = [0]

    def load(src, dst):
        c = pltpu.make_async_copy(src, dst, lsem.at[n_sem[0]])
        n_sem[0] += 1
        c.start()
        return c

    half0 = pl.multiple_of(core * HALF, 128)
    tile0 = (BLK * chip) // 128
    win0 = pl.multiple_of(tile0 * 128, 128)
    off = BLK * chip - win0
    c_x = load(x_hbm, xp.at[pl.ds(0, TOK)])
    c_at = load(at_hbm, at)
    c_hd = load(hd_hbm, hd)
    c_lab = load(lab_hbm, lab)
    c_bmh = load(bm_hbm.at[:, pl.ds(half0, HALF)], bmh)
    c_bmw = load(bm_hbm.at[:, pl.ds(win0, WIN)], bmw)
    c_w1 = [load(w1_hbm.at[:, pl.ds(pl.multiple_of(half0 + a, 128), n)], w1h.at[:, pl.ds(a, n)]) for a, n in W1_CHUNKS]
    c_w2 = [load(w2_hbm.at[pl.ds(a, n), pl.ds(half0, HALF)], w2h.at[pl.ds(a, n)]) for a, n in W2_CHUNKS]
    c_w1w = load(w1_hbm.at[:, pl.ds(win0, WIN)], w1w.at[:, pl.ds(0, WIN)])
    c_w2w = load(w2_hbm.at[:, pl.ds(win0, WIN)], w2w)

    barrier = pltpu.get_barrier_semaphore()
    for m in range(N_CHIP):
        for other in range(N_CORE):
            if m or other:
                pl.semaphore_signal(
                    barrier, inc=1, device_id=(N_CORE * peer(m) + (mate if other else core),), device_id_type=MESH
                )

    eown[...] = jnp.zeros_like(eown)
    row_of_r = (iota((R, R * T), 1) // T == iota((R, R * T), 0)).astype(F32).astype(BF16)
    c_hd.wait()
    for t in range(T):
        v = hd[t].astype(F32)
        for c in range(C):
            hs[pl.ds(c * T + t, 1), :] = v[c : c + 1]
    ha[...] = hs[...].astype(BF16)
    hb[...] = jnp.concatenate([hs[T:, :], hs[:T, :]], axis=0).astype(BF16)
    c_lab.wait()
    lab_f = lab[...].astype(F32)
    eye = (iota((TOK, TOK), 0) == iota((TOK, TOK), 1)).astype(F32).astype(BF16)
    lab_t = nt(eye, jnp.concatenate([lab_f, lab_f], axis=0).astype(BF16))
    onehot = (lab_t == (iota((TOK, C * T), 1) // T).astype(F32)).astype(F32)
    c_x.wait()
    my_row = pl.multiple_of(core * (N_CHIP * TOK) + chip * TOK, TOK)
    xall[pl.ds(my_row, TOK), :] = xp[pl.ds(0, TOK), :]

    pl.semaphore_wait(barrier, N_CHIP * N_CORE - 1)

    k_xp = rcopy(xp.at[pl.ds(0, TOK)], xp.at[pl.ds(TOK, TOK)], ps, pr, chip, mate)
    k_xp.start()
    k_x = {}
    for m in (1, 2, 4, 7):
        k_x[m] = rcopy(xp.at[pl.ds(0, TOK)], xall.at[pl.ds(my_row, TOK)], xs.at[m], xr.at[m], peer(m), core)
        if m != 7:
            k_x[m].start()

    c_at.wait()
    w1w[:, WIN:] = tn(at[...], row_of_r).astype(BF16)
    c_bmw.wait()
    colw = iota((R, WIN), 1)
    bm_f = jnp.where((colw >= off) & (colw < off + BLK), bmw[...].astype(F32), 0.0)
    bmt[...] = tn(bm_f.astype(BF16), row_of_r).astype(BF16)
    first_of_r = (T * iota((R, R * T), 0) == iota((R, R * T), 1)).astype(F32).astype(BF16)
    bms[...] = tn(first_of_r, bmw[...]).astype(BF16)

    k_xp.wait_recv()
    x2 = xp[...]
    u2 = nt(x2, at[...]).astype(BF16)
    c_bmh.wait()
    for (a, n), cp in zip(W1_CHUNKS, c_w1):
        cp.wait()
        for i in range(a, a + n, N_TILE):
            j = min(i + N_TILE, a + n)
            pre = nn(x2, w1h[:, i:j]) + nn(u2, bmh[:, i:j])
            hbuf[:, i:j] = gelu(pre).astype(BF16)
        if a == 1024:
            k_x[7].start()
    k_z = []
    grp_row = pl.multiple_of(core * (N_CHIP * TOK), N_CHIP * TOK)

    def relay():
        for got in (1, 2, 4):
            k_x[got].wait_recv()
        for got, to in ((1, 2), (2, 4), (4, 1)):
            rows = xall.at[pl.ds(pl.multiple_of(grp_row + peer(got) * TOK, TOK), TOK)]
            k_x[got + to] = rcopy(rows, rows, xs.at[got + to], xr.at[got + to], peer(to), core)
            k_x[got + to].start()

    for i, ((a, n), cp) in enumerate(zip(W2_CHUNKS, c_w2)):
        cp.wait()
        for j in range(a, a + n, N_TILE):
            z = nt(hbuf[...], w2h[j : min(j + N_TILE, a + n), :])
            zown[:, j : min(j + N_TILE, a + n)] = z[:TOK]
            zsend[:, j : min(j + N_TILE, a + n)] = z[TOK:]
        k_z.append(rcopy(zsend.at[:, pl.ds(a, n)], zrecv.at[:, pl.ds(a, n)], zs.at[i], zr.at[i], chip, mate))
        k_z[-1].start()
        if i == 0:
            relay()

    c_w1w.wait()

    def slopes(which, base):
        for m in which:
            if m in FAR:
                k_x[m].wait_recv()
        xc = jnp.concatenate(
            [xall[pl.ds(pl.multiple_of(grp_row + peer(m) * TOK, TOK), TOK), :] for m in which], axis=0
        )
        n_row = len(which) * TOK
        last = WIN - WIN % N_TILE
        pre = nn(xc, w1w[:, last:])
        ur = pre[:, WIN - last :].astype(BF16)
        urep[base : base + n_row, :] = ur
        pre = pre[:, : WIN - last] + nn(ur, bms[:, last:])
        g[base : base + n_row, last:] = gelu_slope(pre)
        for a in range(0, last, N_TILE):
            pre = nn(xc, w1w[:, a : a + N_TILE]) + nn(ur, bms[:, a : a + N_TILE])
            g[base : base + n_row, a : a + N_TILE] = gelu_slope(pre)

    slopes(NEAR, 0)
    for k in k_z:
        k.wait_recv()
    xf = xp[pl.ds(0, TOK), :].astype(F32)
    zb = (xf + (zown[...] + zrecv[...])).astype(BF16)
    la, lb = nt(zb, ha[...]), nt(zb, hb[...])
    top = jnp.maximum(la, lb)
    ea, eb = jnp.exp(la - top), jnp.exp(lb - top)
    err = (ea / (ea + eb) - onehot).astype(BF16)
    eown[:, : C * T] = err
    my_slot = pl.multiple_of(chip * TOK, TOK)
    eall[pl.ds(my_slot, TOK), :] = eown[...]
    k_e = {}
    for m in (1, 2, 4, 3, 5, 6, 7):
        k_e[m] = rcopy(eown, eall.at[pl.ds(my_slot, TOK)], es.at[m], er.at[m], peer(m), core)
        k_e[m].start()

    c_w2w.wait()
    lane_t = iota((TOK, R * T), 1) % T
    rel = {m: i * TOK for i, m in enumerate(NEAR + FAR)}
    k_d = {}

    def backward(block):
        for m in block:
            if m:
                k_e[m].wait_recv()
        dus = {}
        for m in block:
            r0 = rel[m] * T
            e = eall[pl.ds(pl.multiple_of(peer(m) * TOK, TOK), TOK), :].astype(F32)
            for t in range(T):
                dz[rel[m] // TOK % 4, t * TOK : (t + 1) * TOK, :] = (
                    e[:, t : t + 1] * hs[pl.ds(t, 1), :] + e[:, T + t : T + t + 1] * hs[pl.ds(T + t, 1), :]
                ).astype(BF16)
            for a in range(0, WIN, N_TILE):
                n = min(N_TILE, WIN - a)
                dh = nn(dz[rel[m] // TOK % 4], w2w[:, a : a + n]).reshape(T, TOK, n)
                slope = g[rel[m] : rel[m] + TOK, a : a + n]
                dp[r0 : r0 + T * TOK, a : a + n] = (dh * slope[None]).astype(BF16).reshape(T * TOK, n)
            du = nn(dp[r0 : r0 + T * TOK, :], bmt[...])
            dus[m] = sum(jnp.where(lane_t == t, du[t * TOK : (t + 1) * TOK], 0.0) for t in range(T))
            if m:
                dsend[m] = dus[m]
            ur = urep[rel[m] : rel[m] + TOK, :].astype(F32)
            for t in range(T):
                ub[r0 + t * TOK : r0 + (t + 1) * TOK, :] = jnp.where(lane_t == t, ur, 0.0).astype(BF16)
        for m in block:
            if m:
                k_d[m] = rcopy(dsend.at[m], drecv.at[m], ds_.at[m], dr.at[m], peer(m), core)
                k_d[m].start()
        return dus

    slopes(FAR, len(NEAR) * TOK)
    k_g = rcopy(xall.at[pl.ds(grp_row, N_CHIP * TOK)], xall.at[pl.ds(grp_row, N_CHIP * TOK)], gs, gr, chip, mate)
    k_g.start()
    for block in BLOCKS[:-1]:
        backward(block)
    du_own = backward(BLOCKS[-1])[0]
    for a in range(0, WIN, N_TILE):
        gb[:, a : min(a + N_TILE, WIN)] = tn(ub[...], dp[:, a : min(a + N_TILE, WIN)])

    ow0 = pl.multiple_of(core * (OWIN - 128), 128)
    mw0 = pl.multiple_of(mate * (OWIN - 128), 128)
    k_b = rcopy(gb.at[:, pl.ds(mw0, OWIN)], gbrecv, bs, br, chip, mate)
    k_b.start()
    for m in range(1, N_CHIP):
        k_d[m].wait_recv()
        du_own = du_own + drecv[m]
    duown[...] = du_own.astype(BF16)
    duall[pl.ds(my_row, TOK), :] = duown[...]
    others = [(m, o) for m in (7, 6, 5, 3, 4, 2, 1, 0) for o in range(N_CORE) if m or o]
    k_n = []
    for i, (m, o) in enumerate(others):
        k_n.append(rcopy(duown, duall.at[pl.ds(my_row, TOK)], ns.at[i], nr.at[i], peer(m), mate if o else core))
        k_n[-1].start()

    k_b.wait_recv()
    off_own = off + 16 * core
    colo = iota((R * T, OWIN), 1)
    shard = (gb[:, pl.ds(ow0, OWIN)] + gbrecv[...]) * (1.0 / (N_CHIP * N_CORE * TOK))
    shard = jnp.where((colo >= off_own) & (colo < off_own + OWN), shard, 0.0)
    gbrecv[...] = shard
    lane = iota((T, 128), 1)
    sub = iota((T, 128), 0)
    parts = gram_parts([gbrecv[r * T : (r + 1) * T, :] for r in range(R)])
    row = sum(
        jnp.where(lane == T * k + sub, jnp.sum(p, axis=1, keepdims=True), 0.0) for k, p in enumerate(parts)
    )
    mown[...] = jnp.sum(row, axis=0, keepdims=True)
    mall[me] = mown[...]
    k_m = []
    for i, (m, o) in enumerate(others):
        k_m.append(rcopy(mown, mall.at[me], ms.at[i], mr.at[i], peer(m), mate if o else core))
        k_m[-1].start()

    k_g.wait_recv()
    for k in k_n:
        k.wait_recv()
    ga[:, :D] = tn(duall[...], xall[...]) * (1.0 / (N_CHIP * N_CORE * TOK))
    ga[:, D:] = jnp.zeros((R * T, DP - D), F32)
    parts = gram_parts([ga[r * T : (r + 1) * T, :] for r in range(R)])
    for k in k_m:
        k.wait_recv()
    mb = jnp.broadcast_to(sum(mall[i] for i in range(N_CHIP * N_CORE)), (T, 128))
    col = [
        jnp.sum(p + jnp.where(lane == T * k + sub, mb, 0.0), axis=1, keepdims=True) + jnp.zeros((T, 128), F32)
        for k, p in enumerate(parts)
    ]
    scale = jnp.sum(col[0], axis=0, keepdims=True) / T
    col = [c / scale for c in col]
    col += [pltpu.roll(col[T - k], k, 0) for k in range(5, T)]

    def eg_step(_, w):
        grad = sum(col[k] * (w if k == 0 else pltpu.roll(w, k, 0)) for k in range(T))
        w = w * jnp.exp(-grad)
        return w / jnp.sum(w, axis=0, keepdims=True)

    w = lax.fori_loop(0, EG_STEPS, eg_step, jnp.full((T, 128), 1.0 / T, F32))
    alpha_out[...] = jnp.sum(jnp.where(lane == sub, w, 0.0), axis=0, keepdims=True)[:, :T]

    wcol = w[:, 0:1]
    dstart = (D // (N_CHIP * N_CORE)) * me
    dtile = dstart // 128
    da0 = pl.multiple_of(dtile * 128, 128)
    comb_a = jnp.concatenate(
        [jnp.sum(ga[r * T : (r + 1) * T, pl.ds(da0, 256)] * wcol, axis=0, keepdims=True) for r in range(R)], axis=0
    )
    ga_out[...] = pltpu.roll(comb_a, 256 - (dstart - da0), 1)[:, : D // (N_CHIP * N_CORE)]
    comb_b = jnp.concatenate(
        [jnp.sum(gbrecv[r * T : (r + 1) * T, :] * wcol, axis=0, keepdims=True) for r in range(R)], axis=0
    )
    gb_out[...] = pltpu.roll(comb_b, OWIN - off_own, 1)[:, :OWN]

    for k in [k_xp, k_g, k_b] + k_z + k_n + k_m + [k_x[m] for m in k_x] + [k_e[m] for m in k_e] + [k_d[m] for m in k_d]:
        k.wait_send()


def put_kernel(alpha_in, ga_in, gb_in, alpha_out, ga_out, gb_out, sem):
    pairs = ((alpha_in, alpha_out), (ga_in, ga_out), (gb_in, gb_out))
    copies = [pltpu.make_async_copy(a, b, sem.at[i]) for i, (a, b) in enumerate(pairs)]
    for c in copies:
        c.start()
    for c in copies:
        c.wait()


def solution(mesh):
    n_dev = mesh.shape["data"]
    assert n_dev == N_CHIP * N_CORE
    vm = pltpu.VMEM
    dma = pltpu.SemaphoreType.DMA
    scratch = [
        vm((D, HALF), BF16), vm((D, HALF), BF16), vm((D, WIN + R * T), BF16), vm((D, WIN), BF16),
        vm((R, HALF), BF16), vm((R, WIN), BF16), vm((R, D), BF16), vm((T, C, D), BF16), vm((T, TOK), jnp.int32),
        vm((2 * TOK, D), BF16), vm((n_dev * TOK, D), BF16), vm((2 * TOK, HALF), BF16),
        vm((C * T, D), F32), vm((C * T, D), BF16), vm((C * T, D), BF16),
        vm((WIN, R * T), BF16), vm((R * T, WIN), BF16),
        vm((N_CHIP * TOK, R * T), BF16), vm((N_CHIP * TOK, WIN), F32),
        vm((TOK, D), F32), vm((TOK, D), F32), vm((TOK, D), F32),
        vm((TOK, 128), BF16), vm((N_CHIP * TOK, 128), BF16),
        vm((4, T * TOK, D), BF16), vm((N_CHIP * T * TOK, WIN), BF16), vm((N_CHIP * T * TOK, R * T), BF16),
        vm((N_CHIP, TOK, R * T), F32), vm((N_CHIP, TOK, R * T), F32),
        vm((TOK, R * T), BF16), vm((n_dev * TOK, R * T), BF16),
        vm((R * T, WIN), F32), vm((R * T, OWIN), F32),
        vm((1, 128), F32), vm((n_dev, 1, 128), F32), vm((R * T, DP), F32),
        dma((16,)), dma((N_CHIP,)), dma((N_CHIP,)), dma, dma, dma((4,)), dma((4,)),
        dma((N_CHIP,)), dma((N_CHIP,)), dma((N_CHIP,)), dma((N_CHIP,)), dma, dma,
        dma((n_dev,)), dma((n_dev,)), dma((n_dev,)), dma((n_dev,)), dma, dma,
    ]

    def device_step(tokens, labels, w_one, w_two, adapter_a, adapter_b, task_heads):
        out_shapes = ((1, T), (R, D // n_dev), (R, FF // n_dev))
        call = pl.pallas_call(
            kernel,
            out_shape=tuple(pltpu.VMEM(s, F32) for s in out_shapes),
            in_specs=[pl.BlockSpec(memory_space=pltpu.HBM)] * 7,
            out_specs=tuple([pl.BlockSpec(memory_space=pltpu.VMEM)] * 3),
            scratch_shapes=scratch,
            compiler_params=pltpu.CompilerParams(
                collective_id=0, has_side_effects=True, vmem_limit_bytes=60 * 1024 * 1024
            ),
            name="min_norm",
        )
        put = pl.pallas_call(
            put_kernel,
            out_shape=tuple(jax.ShapeDtypeStruct(s, F32) for s in out_shapes),
            in_specs=[pl.BlockSpec(memory_space=pltpu.VMEM)] * 3,
            out_specs=tuple([pl.BlockSpec(memory_space=pltpu.HBM)] * 3),
            scratch_shapes=[dma((3,))],
            compiler_params=pltpu.CompilerParams(vmem_limit_bytes=1024 * 1024),
            name="put",
        )
        results = call(
            tokens, labels, w_one, w_two.T, adapter_a.T, adapter_b, task_heads.transpose(0, 2, 1)
        )
        alpha, ga_t, gb = put(*results)
        return alpha.reshape(T), ga_t.T, gb

    return jax.shard_map(
        device_step,
        mesh=mesh,
        in_specs=(P("data", None), P(None, "data"), P(), P(), P(), P(), P()),
        out_specs=(P(), P("data", None), P(None, "data")),
        check_vma=False,
    )
```
